32 devices in a mesh: row: 8 (over z, core), col: 4 (over y, x).
Axes of the slice: x: 2, y: 2, z: 4, core: 2. Of those that a mesh axis runs over, the one named last changes fastest.
Arguments:
- object_field: float32 [3, 2, 1024, 512], P(None, None, 'row', 'col'), may hold values from -5 to 5
- probe: float32 [2, 128, 128], replicated, may hold values from -5 to 5
- measured: float32 [8, 4, 2, 128, 128], P('row', 'col'), may hold values from 0.25 to 4
- positions: int32 [8, 4, 2, 2], P('row', 'col'), may hold values from 0 to 127
- counts: int32 [8, 4], P('row', 'col'), may hold values from 1 to 2, as said below
Outputs:
- object_next: float32 [3, 2, 1024, 512], P(None, None, 'row', 'col')
The draws below stay inside these ranges and needn't reach their ends.
Inputs may be any that keep to these rules, and one draw needn't show every extreme that they name: Slots 0 to counts - 1 of a tile are live; some tile has all 2 live.
All inputs are finite; a program needn't handle non-finite values.
Results may differ from the reference program's by a relative error of at most 0.0003.
Values sent between devices are 32-bit elements; how exact they have to be, the bound alone decides.
A program may use at most 64 MiB of HBM per device.

```python
import math
import jax
import jax.numpy as jnp
from jax import lax

W = 128
S = 128
SLICES = 3
ITERS = 2
SLOTS = 2
TILE_ROWS = 8
TILE_COLS = 4
ROWS_ALL = 1024
COLS_ALL = 512


def draw_counts(key, part):
    first_key = jax.random.fold_in(key, 11)
    second_key = jax.random.fold_in(key, 12)
    third_key = jax.random.fold_in(key, 13)
    first_draw = jax.random.randint(first_key, (TILE_ROWS, TILE_COLS), 1, SLOTS + 1, dtype=jnp.int32)
    second_draw = jax.random.randint(second_key, (TILE_ROWS, TILE_COLS), 1, SLOTS + 1, dtype=jnp.int32)
    busiest = jax.random.randint(third_key, (), 0, TILE_ROWS * TILE_COLS, dtype=jnp.int32)
    ordinal = jnp.arange(TILE_ROWS * TILE_COLS, dtype=jnp.int32).reshape(TILE_ROWS, TILE_COLS)
    return jnp.where(ordinal == busiest, SLOTS, jnp.minimum(first_draw, second_draw)).astype(jnp.int32)


def place_ends(entries, key, least, high):
    longest = entries.shape.index(max(entries.shape))
    spots = []
    for shift in (0, 1):
        where = [jax.random.randint(jax.random.fold_in(key, axis), (), 0, length) for axis, length in enumerate(entries.shape)]
        where[longest] = (where[longest] + shift) % entries.shape[longest]
        spots.append(tuple(where))
    return entries.at[spots[0]].set(least).at[spots[1]].set(high)


def steps_of(rng, extent, split, low, largest):
    def one(dim, parts):
        steps = jax.random.uniform(jax.random.fold_in(jax.random.fold_in(rng, 6), dim), (parts,), jnp.float32, low / len(split), largest / len(split))
        return jnp.repeat(jnp.exp(steps), extent[dim] // parts).reshape((-1,) + (1,) * (len(extent) - dim - 1))

    factor_of = one(*split[0])
    for cut in split[1:]:
        factor_of = factor_of * one(*cut)
    return factor_of


def centred(stream_key, shape, scale, reach, shards=(), kind=jnp.bfloat16):
    drawn = scale * jax.random.normal(stream_key, shape, jnp.float32)
    if shards:
        drawn = drawn * steps_of(stream_key, shape, shards, -0.22, 0.18)
    return jnp.clip(drawn, -reach, reach).astype(kind)


def setup_inputs(seed: int = 0) -> dict:
    streams_of = jax.random.split(jax.random.key(seed), 6)
    return {
        "object_field": centred(streams_of[0], (SLICES, 2, ROWS_ALL, COLS_ALL), 0.7, 5.0, ((2, 8), (3, 4)), jnp.float32),
        "probe": centred(streams_of[1], (2, W, W), 0.7, 5.0, (), jnp.float32),
        "measured": jnp.clip(jnp.exp(math.log(4.0) - 2.7725887 * jax.random.uniform(streams_of[2], (TILE_ROWS, TILE_COLS, SLOTS, W, W), jnp.float32) ** steps_of(streams_of[2], (TILE_ROWS, TILE_COLS, SLOTS, W, W), ((0, 8), (1, 4)), -0.2, 0.2)), 0.25, 4.0),
        "positions": place_ends(jax.random.randint(streams_of[3], (TILE_ROWS, TILE_COLS, SLOTS, 2), 0, S), jax.random.fold_in(streams_of[3], 1), 0, S - 1).astype(jnp.int32),
        "counts": draw_counts(jax.random.fold_in(streams_of[5], 71), 0),
    }


LEARNING_RATE = 0.02


def phase_table():
    frequency = (jnp.arange(W, dtype=jnp.int32) + W // 2) % W - W // 2
    squares = (frequency[:, None] * frequency[:, None] + frequency[None, :] * frequency[None, :]).astype(jnp.float32)
    angles = (-0.25 * math.pi / W) * squares
    return lax.complex(jnp.cos(angles), jnp.sin(angles))


def propagate(wavefield, kernel):
    return jnp.fft.ifft2(jnp.fft.fft2(wavefield, norm="ortho") * kernel, norm="ortho")


def window_gradient(window, probe_wave, sample, kernel):
    layers = [lax.complex(window[slice_index, 0], window[slice_index, 1]) for slice_index in range(SLICES)]
    wavefield = probe_wave
    incident = []
    for slice_index in range(SLICES):
        incident.append(wavefield)
        wavefield = layers[slice_index] * wavefield
        if slice_index + 1 < SLICES:
            wavefield = propagate(wavefield, kernel)
    far_field = jnp.fft.fft2(wavefield, norm="ortho")
    residue = jnp.real(far_field) ** 2 + jnp.imag(far_field) ** 2 - sample
    back_wave = jnp.fft.ifft2(residue * far_field, norm="ortho")
    pieces = [None] * SLICES
    for slice_index in reversed(range(SLICES)):
        product = jnp.conj(incident[slice_index]) * back_wave
        pieces[slice_index] = jnp.stack([jnp.real(product), jnp.imag(product)])
        if slice_index > 0:
            back_wave = propagate(jnp.conj(layers[slice_index]) * back_wave, jnp.conj(kernel))
    return jnp.stack(pieces)


def reference(object_field, probe, measured, positions, counts):
    rim_width = W // 2
    kernel = phase_table()
    probe_wave = lax.complex(probe[0], probe[1])
    total_windows = TILE_ROWS * TILE_COLS * SLOTS
    flat_corners = positions.reshape(total_windows, 2).astype(jnp.int32)
    flat_samples = measured.reshape(total_windows, W, W)
    ordinal = jnp.arange(total_windows, dtype=jnp.int32)
    tile_number = ordinal // SLOTS
    live_mask = (ordinal % SLOTS < counts.reshape(-1).astype(jnp.int32)[tile_number]).astype(object_field.dtype)
    row_start = ((tile_number // TILE_COLS) * S + flat_corners[:, 0]).astype(jnp.int32)
    col_start = ((tile_number % TILE_COLS) * S + flat_corners[:, 1]).astype(jnp.int32)
    anchor = jnp.zeros((), jnp.int32)
    current = object_field
    for iteration in range(ITERS):
        padded = jnp.pad(current, ((0, 0), (0, 0), (rim_width, rim_width), (rim_width, rim_width)))

        def visit(window_index, running):
            corner_start = (anchor, anchor, row_start[window_index], col_start[window_index])
            window = lax.dynamic_slice(padded, corner_start, (SLICES, 2, W, W))
            update = window_gradient(window, probe_wave, flat_samples[window_index], kernel) * live_mask[window_index]
            before = lax.dynamic_slice(running, corner_start, (SLICES, 2, W, W))
            return lax.dynamic_update_slice(running, before + update.astype(running.dtype), corner_start)

        gradient_sum = lax.fori_loop(0, total_windows, visit, jnp.zeros_like(padded))
        interior = gradient_sum[:, :, rim_width:rim_width + TILE_ROWS * S, rim_width:rim_width + TILE_COLS * S]
        current = current - LEARNING_RATE * interior
    return current
```

```python
import functools

import jax
import jax.numpy as jnp
import ml_dtypes
import numpy as np
from jax import lax
from jax.experimental import pallas as pl
from jax.experimental.pallas import tpu as pltpu
from jax.sharding import PartitionSpec as P

LEARNING_RATE = 0.02
COPIES = 192


def halves_of(matrix):
    block = np.block([[matrix.real, matrix.imag], [-matrix.imag, matrix.real]])
    block = block.astype(np.float32)
    lead = block.astype(ml_dtypes.bfloat16)
    trail = (block - lead.astype(np.float32)).astype(ml_dtypes.bfloat16)
    return np.stack([lead, trail])


def make_tables(side):
    ordinal = np.arange(side)
    fourier = np.exp(-2j * np.pi / side * (np.outer(ordinal, ordinal) % side)) / np.sqrt(side)
    frequency = (ordinal + side // 2) % side - side // 2
    phase = np.exp(-0.25j * np.pi / side * frequency * frequency)
    spread = (fourier.conj() * phase[None, :]) @ fourier
    forms = [fourier, fourier.conj(), spread, spread.conj()]
    return np.stack([halves_of(form) for form in forms])


def split(values):
    lead = values.astype(jnp.bfloat16)
    return lead, (values - lead.astype(jnp.float32)).astype(jnp.bfloat16)


def dot(left, right):
    return jnp.dot(left, right, preferred_element_type=jnp.float32)


def both_sides(waves, table, form):
    side = waves[0][0].shape[0]
    stacked = jnp.concatenate([jnp.concatenate(pair, axis=1) for pair in waves], axis=0)
    lead, trail = split(stacked)
    right = (table[form, 0], table[form, 1])
    out = dot(lead, right[0]) + dot(trail, right[0]) + dot(lead, right[1])
    count = len(waves)
    turned = jnp.concatenate(
        [
            jnp.concatenate(
                [out[w * side : (w + 1) * side, part * side : (part + 1) * side] for w in range(count)],
                axis=1,
            )
            for part in range(2)
        ],
        axis=0,
    )
    lead, trail = split(turned)
    left = (table[form ^ 1, 0], table[form ^ 1, 1])
    out = dot(left[0], lead) + dot(left[0], trail) + dot(left[1], lead)
    return [
        tuple(
            out[part * side : (part + 1) * side, w * side : (w + 1) * side] for part in range(2)
        )
        for w in range(count)
    ]


def times(a, b):
    return (a[0] * b[0] - a[1] * b[1], a[0] * b[1] + a[1] * b[0])


def conj_times(a, b):
    return (a[0] * b[0] + a[1] * b[1], a[0] * b[1] - a[1] * b[0])


def pack(tile):
    half = tile.shape[0] // 2
    lane = lax.broadcasted_iota(jnp.int32, (half, tile.shape[1]), 1)
    low, high = tile[:half], tile[half:]
    left = jnp.where(lane < half, low, pltpu.roll(high, half, 1))
    right = jnp.where(lane < half, pltpu.roll(low, half, 1), high)
    return left, right


def unpack(left, right):
    half = left.shape[0]
    lane = lax.broadcasted_iota(jnp.int32, left.shape, 1)
    low = jnp.where(lane < half, left, pltpu.roll(right, half, 1))
    high = jnp.where(lane < half, pltpu.roll(left, half, 1), right)
    return jnp.concatenate([low, high], axis=0)


def step_kernel(
    shape, field, probe, samples, corners, count, table_far, out,
    table, near, near_samples, near_corners, near_count, far_out, far_in, wide, tall,
    grads, grads_in, later, kept, grad_rows, grad_in, grad_cols, fold_in, relay,
    send_sem, recv_sem, table_sem,
):
    layer_count = field.shape[0]
    side = field.shape[-1]
    slots = samples.shape[0]
    half = side // 2
    slices = range(layer_count)
    row, col = lax.axis_index("row"), lax.axis_index("col")
    rows_all, cols_all = shape["row"], shape["col"]
    has_row = (row > 0, row < rows_all - 1)
    has_col = (col > 0, col < cols_all - 1)
    has_far = (col > 1, col < cols_all - 2)
    parts = (pl.ds(0, half), pl.ds(half, half))
    detour = cols_all == 4
    started = []
    numbers = {}

    def both(a, b):
        return jnp.logical_and(a, b)

    def passed_on(d):
        return (col == 2 - d) if detour else None

    def outer(d):
        return col == (3 if d else 0)

    def here(there, d):
        return both(there, jnp.logical_not(passed_on(d))) if detour else there

    def copy(key, src, dst, axis="col", step=0, passes=False):
        number = numbers.setdefault(key, len(numbers))
        sent = numbers.setdefault(key + ("passed",), len(numbers)) if passes else number
        return pltpu.make_async_remote_copy(
            src_ref=src,
            dst_ref=dst,
            send_sem=send_sem.at[sent],
            recv_sem=recv_sem.at[number],
            device_id={axis: (row if axis == "row" else col) + step},
            device_id_type=pl.DeviceIdType.MESH,
        )

    def start(when, moved):
        pl.when(when)(moved.start)
        started.append((when, moved))

    def arrive(when, moved):
        pl.when(when)(moved.wait_recv)

    def chunk(ref, k):
        return ref.at[0] if k == 0 else ref.at[1, parts[k - 1]]

    def near_copy(s, k, d, step=None, src=None):
        passes = src is not None
        src = src if passes else chunk(field.at[s], k)
        dst = chunk(near.at[1 - d, s], k)
        step = step if passes else 1 if d else -1
        return copy(("near", s, k, d), src, dst, "col", step, passes)

    def lend_copy(s, d):
        return copy(("lend", s), chunk(field.at[s], 2), relay.at[0, s], "col", 2 if d else -2)

    def samples_copy(d, step=None, src=None):
        passes = src is not None
        step = step if passes else 1 if d else -1
        src = src if passes else samples
        return copy(("samples", d), src, near_samples.at[1 - d], "col", step, passes)

    def corners_copy(d):
        return copy(("corners", d), corners.at[0, 0], near_corners.at[1 - d], "col", 1 if d else -1)

    def count_copy(d):
        return copy(("count", d), count, near_count.at[1 - d], "col", 1 if d else -1)

    def far_copy(s, d):
        return copy(("far", s, d), far_out.at[d, s], far_in.at[d, s], "col", 2 if d else -2)

    def tall_copy(i, s, d):
        ref = (field, near.at[0], near.at[1], wide)[i]
        src, dst = ref.at[s, :, parts[d]], tall.at[i, s, :, parts[d]]
        return copy(("tall", i, s, d), src, dst, "row", 1 if d else -1)

    def grads_copy(s, a, d):
        rows = parts[d ^ a]
        src, dst = grads.at[s, a, :, :, rows], grads_in.at[s, 1 - a, :, :, rows]
        return copy(("grads", s, a, d), src, dst, "row", 1 if d else -1)

    def fold_rows_copy(s, b, d):
        rows = parts[1 - d]
        src, dst = grad_rows.at[s, b, :, rows], grad_in.at[s, b, :, rows]
        return copy(("fold_rows", s, b, d), src, dst, "row", 1 if d else -1)

    def fold_cols_copy(s, part, d, leg=0):
        key = ("fold_cols", s, part, d)
        src, dst = grad_cols.at[1 - d, s, part], fold_in.at[1 - d, s, part]
        step = 1 if d else -1
        if leg == 0:
            return copy(key, src, dst, "col", step)
        held = relay.at[1, s]
        if leg == 1:
            return copy(("lend_cols", s), src, held, "col", 2 * step)
        return copy(key, held, dst, "col", -step)

    load = pltpu.make_async_copy(table_far, table, table_sem)
    load.start()
    barrier = pltpu.get_barrier_semaphore()
    meets = [("row", 1 if d else -1, has_row[d]) for d in range(2)]
    meets += [("col", 1 if d else -1, has_col[d]) for d in range(2)]
    meets += [("col", 2 if d else -2, has_far[d]) for d in range(2)]
    for axis, step, there in meets:

        @pl.when(there)
        def greet():
            pl.semaphore_signal(
                barrier,
                inc=1,
                device_id={axis: (row if axis == "row" else col) + step},
                device_id_type=pl.DeviceIdType.MESH,
            )

    pl.semaphore_wait(barrier, sum(there.astype(jnp.int32) for _, _, there in meets))

    def ship_near(s):
        for k in range(3):
            for d in range(2):
                start(here(has_col[d], d), near_copy(s, k, d))

    def ship_far(s):
        for part in range(2):
            for d, piece in enumerate(pack(field[s, part])):
                far_out[d, s, part] = piece
        for d in range(2):
            start(has_far[d], far_copy(s, d))
            if detour:
                start(passed_on(d), lend_copy(s, d))

    def hand_lent(s):
        if detour:
            for d in range(2):
                away = outer(d)
                arrive(away, lend_copy(s, d))
                start(away, near_copy(s, 2, d, -1 if d else 1, relay.at[0, s]))

    def hand_near(s):
        if detour:
            for k in range(2):
                for d in range(2):
                    away = outer(1 - d)
                    arrive(away, near_copy(s, k, 1 - d))
                    src = chunk(near.at[d, s], k)
                    start(away, near_copy(s, k, d, 2 if d else -2, src))

    def hand_samples():
        if detour:
            for d in range(2):
                away = outer(1 - d)
                arrive(away, samples_copy(1 - d))
                start(away, samples_copy(d, 2 if d else -2, near_samples.at[d]))

    def ship_samples(mine):
        for d in range(2):
            when = here(has_col[d], d)
            start(when if mine is None else both(when, mine), samples_copy(d))

    for d in range(2):
        start(has_col[d], corners_copy(d))
        start(has_col[d], count_copy(d))
    for s in slices:
        if s < 2:
            ship_near(s)
        for d in range(2):
            start(has_row[d], tall_copy(0, s, d))
        ship_far(s)

    def clear(when, *refs):
        @pl.when(jnp.logical_not(when))
        def fill():
            for ref in refs:
                ref[...] = jnp.zeros(ref.shape, ref.dtype)

    for d in range(2):
        clear(has_col[d], near.at[d], near_samples.at[d], tall.at[1 + d], fold_in.at[d])
        clear(has_far[1 - d], far_in.at[d])
        rows = parts[1 - d]
        for s in slices:
            clear(has_row[d], tall.at[0, s, :, rows], tall.at[3, s, :, rows])
            clear(has_row[d], tall.at[1, s, :, rows], tall.at[2, s, :, rows])
            clear(has_row[d], grads_in.at[s, 0, :, :, parts[d]], grads_in.at[s, 1, :, :, rows])
            clear(has_row[d], grad_in.at[s, :, :, parts[d]])

        @pl.when(jnp.logical_not(has_col[d]))
        def nobody():
            near_count[d, 0, 0] = 0
            for j in range(slots):
                for dim in range(2):
                    near_corners[d, j, dim] = 0

    lane = lax.broadcasted_iota(jnp.int32, (side, side), 1)
    first = lane < half

    class Window:
        pass

    def corner_of(k, j, dim):
        return corners[0, 0, j, dim] if k == 1 else near_corners[k // 2, j, dim]

    def window_of(k, j):
        found = Window()
        found.tile, found.slot = k, j
        masks = []
        for dim in range(2):
            place = lax.broadcasted_iota(jnp.int32, (side, side), dim)
            corner = corner_of(k, j, dim)
            masks.append((place >= corner + half) | (place < corner - half))
        found.rows, found.cols = masks
        shifts = [lax.rem(corner_of(k, j, dim) + half, side) for dim in range(2)]
        found.beam = tuple(
            pltpu.roll(pltpu.roll(probe[part], shifts[0], 0), shifts[1], 1) for part in range(2)
        )
        found.live = j < (count[0, 0] if k == 1 else near_count[k // 2, 0, 0])
        return found

    for d in range(2):
        arrive(has_col[1 - d], corners_copy(d))
        arrive(has_col[1 - d], count_copy(d))
    own_windows = [window_of(1, j) for j in range(slots)]
    side_windows = [window_of(k, j) for k in (0, 2) for j in range(slots)]
    load.wait()

    def relay_on(s):
        hand_lent(s)
        hand_near(s)

    def ship_tall(s):
        for d in range(2):
            for k in range(3):
                mine = has_col[1 - d]
                if detour and k < 2:
                    mine = both(mine, jnp.logical_not(outer(d)))
                arrive(mine, near_copy(s, k, d))
        for d in range(2):
            for e in range(2):
                start(both(has_row[d], has_col[e]), tall_copy(1 + e, s, d))
        for d in range(2):
            arrive(has_far[1 - d], far_copy(s, d))
        for part in range(2):
            wide[s, part] = unpack(far_in[0, s, part], far_in[1, s, part])
        for d in range(2):
            start(has_row[d], tall_copy(3, s, d))

    def land_tall(s):
        for i in range(4):
            for d in range(2):
                there = has_row[1 - d] if i in (0, 3) else both(has_row[1 - d], has_col[i - 1])
                arrive(there, tall_copy(i, s, d))

    def spread(tiles, beyond, k):
        if k == 1:
            return jnp.where(first, tiles[2], tiles[0])
        return jnp.where(first, tiles[1], beyond) if k == 0 else jnp.where(first, beyond, tiles[1])

    def cut(w, inner, across, down, slant):
        return tuple(
            jnp.where(
                w.rows,
                jnp.where(w.cols, slant[part], down[part]),
                jnp.where(w.cols, across[part], inner[part]),
            )
            for part in range(2)
        )

    def layers_first(s, windows):
        pieces = {}
        for k in range(3):
            tiles = [[near[0, s, p], field[s, p], near[1, s, p]] for p in range(2)]
            talls = [[tall[1, s, p], tall[0, s, p], tall[2, s, p]] for p in range(2)]
            pieces[k] = (
                [tiles[p][k] for p in range(2)],
                [spread(tiles[p], wide[s, p], k) for p in range(2)],
                [talls[p][k] for p in range(2)],
                [spread(talls[p], tall[3, s, p], k) for p in range(2)],
            )
        return [cut(w, *pieces[w.tile]) for w in windows]

    def residues(far, windows):
        scaled = []
        for w, value in zip(windows, far, strict=True):
            seen = samples[w.slot] if w.tile == 1 else near_samples[w.tile // 2, w.slot]
            residue = value[0] * value[0] + value[1] * value[1] - seen
            scaled.append((residue * value[0], residue * value[1]))
        return scaled

    def gather_first(s, windows, pieces):
        keep = jnp.zeros((side, side), jnp.float32)
        for part in range(2):
            totals = [[keep, keep], [keep, keep]]
            for w, piece in zip(windows, pieces, strict=True):
                value = jnp.where(w.live, piece[part], 0.0)
                inner, outside = jnp.where(w.cols, 0.0, value), jnp.where(w.cols, value, 0.0)
                if w.tile == 0:
                    inner, outside = jnp.where(first, outside, 0.0), jnp.where(first, 0.0, inner)
                elif w.tile == 2:
                    inner, outside = jnp.where(first, 0.0, outside), jnp.where(first, inner, 0.0)
                for b, share in enumerate((inner, outside)):
                    totals[0][b] += jnp.where(w.rows, 0.0, share)
                    totals[1][b] += jnp.where(w.rows, share, 0.0)
            for a in range(2):
                for b in range(2):
                    grads[s, a, b, part] = totals[a][b]

    def send_grads(s, a):
        for d in range(2):
            start(has_row[d], grads_copy(s, a, d))

    def renew(s):
        for a in range(2):
            for d in range(2):
                arrive(has_row[1 - d], grads_copy(s, a, d))
        top = lax.broadcasted_iota(jnp.int32, (side, side), 0) < half
        in_cols = jnp.where(first, has_col[1].astype(jnp.int32), has_col[0].astype(jnp.int32)) > 0
        in_rows = jnp.where(top, has_row[1].astype(jnp.int32), has_row[0].astype(jnp.int32)) > 0
        for part in range(2):
            tiles = [near[0, s, part], field[s, part], near[1, s, part]]
            talls = [tall[1, s, part], tall[0, s, part], tall[2, s, part]]
            before = [[tiles[1], spread(tiles, None, 1)], [talls[1], spread(talls, None, 1)]]
            for a in range(2):
                for b in range(2):
                    total = grads[s, a, b, part] + grads_in[s, a, b, part]
                    value = before[a][b] - LEARNING_RATE * total
                    if b:
                        value = jnp.where(in_cols, value, 0.0)
                    if a:
                        value = jnp.where(in_rows, value, 0.0)
                    later[a, b, s, part] = value

    def layers_second(s, windows):
        pieces = [[later[a, b, s, part] for part in range(2)] for a in range(2) for b in range(2)]
        return [cut(w, *pieces) for w in windows]

    windows = own_windows + side_windows
    waves = [w.beam for w in windows]
    incident, layers = [], []
    relay_on(0)
    for s in range(2, layer_count):
        ship_near(s)
    ends = jnp.logical_or(outer(0), outer(1))
    ship_samples(jnp.logical_not(ends) if detour else None)
    ship_tall(0)
    for s in range(1, layer_count):
        hand_lent(s)
    if detour:
        ship_samples(ends)
    for s in slices:
        if s + 1 < layer_count:
            hand_near(s + 1)
            ship_tall(s + 1)
        else:
            hand_samples()
        land_tall(s)
        incident.append(waves)
        layers.append(layers_first(s, windows))
        waves = [times(layer, wave) for layer, wave in zip(layers[s], waves, strict=True)]
        if s + 1 < layer_count:
            waves = both_sides(waves, table, 2)
    far = both_sides(waves, table, 0)
    for d in range(2):
        mine = has_col[1 - d]
        arrive(both(mine, jnp.logical_not(outer(d))) if detour else mine, samples_copy(d))
    back = both_sides(residues(far, windows), table, 1)
    for s in reversed(slices):
        pieces = [conj_times(a, b) for a, b in zip(incident[s], back, strict=True)]
        gather_first(s, windows, pieces)
        send_grads(s, 0)
        if s > 0:
            moved = [conj_times(a, b) for a, b in zip(layers[s], back, strict=True)]
            back = both_sides(moved, table, 3)
    for s in slices:
        send_grads(s, 1)

    windows = own_windows
    waves = [w.beam for w in windows]
    incident, layers = [], []
    for s in slices:
        renew(s)
        incident.append(waves)
        layers.append(layers_second(s, windows))
        waves = [times(layer, wave) for layer, wave in zip(layers[s], waves, strict=True)]
        if s + 1 < layer_count:
            waves = both_sides(waves, table, 2)
    far = both_sides(waves, table, 0)
    back = both_sides(residues(far, windows), table, 1)

    def gather_second(s, pieces):
        for part in range(2):
            totals = [[0.0, 0.0], [0.0, 0.0]]
            for w, piece in zip(windows, pieces, strict=True):
                value = jnp.where(w.live, piece[part], 0.0)
                by_rows = (jnp.where(w.rows, 0.0, value), jnp.where(w.rows, value, 0.0))
                for a in range(2):
                    totals[a][0] += jnp.where(w.cols, 0.0, by_rows[a])
                    totals[a][1] += jnp.where(w.cols, by_rows[a], 0.0)
            for b in range(2):
                kept[b, s, part] = totals[0][b]
                grad_rows[s, b, part] = totals[1][b]
        for d in range(2):
            start(has_row[d], fold_rows_copy(s, 1, d))

    def ship_cols(s):
        for d in range(2):
            arrive(has_row[1 - d], fold_rows_copy(s, 1, d))
        for part in range(2):
            aside = kept[1, s, part] + grad_in[s, 1, part]
            for d, piece in enumerate(pack(aside)):
                grad_cols[d, s, part] = piece
        for part in (1, 0):
            for d in range(2):
                when = here(has_col[d], d) if part else has_col[d]
                start(when, fold_cols_copy(s, part, d))
                if detour and part:
                    start(passed_on(d), fold_cols_copy(s, part, d, 1))

    def hand_cols(s):
        if detour:
            for d in range(2):
                arrive(outer(d), fold_cols_copy(s, 1, d, 1))
                start(outer(d), fold_cols_copy(s, 1, d, 2))

    def finish(s):
        for d in range(2):
            arrive(has_row[1 - d], fold_rows_copy(s, 0, d))
            for part in range(2):
                arrive(has_col[1 - d], fold_cols_copy(s, part, d))
        for part in range(2):
            inner = kept[0, s, part] + grad_in[s, 0, part]
            total = inner + unpack(fold_in[0, s, part], fold_in[1, s, part])
            out[s, part] = later[0, 0, s, part] - LEARNING_RATE * total

    for s in reversed(slices):
        gather_second(s, [conj_times(a, b) for a, b in zip(incident[s], back, strict=True)])
        if s + 1 < layer_count:
            ship_cols(s + 1)
        if s > 0:
            moved = [conj_times(a, b) for a, b in zip(layers[s], back, strict=True)]
            back = both_sides(moved, table, 3)
    for s in reversed(slices):
        for d in range(2):
            start(has_row[d], fold_rows_copy(s, 0, d))
    for s in range(layer_count - 1, 1, -1):
        hand_cols(s)
    ship_cols(0)
    for s in reversed(range(min(2, layer_count))):
        hand_cols(s)
    for s in reversed(slices):
        finish(s)
    for when, moved in started:
        pl.when(when)(moved.wait_send)
    assert len(numbers) <= COPIES


def shards(shape, object_field, probe, measured, positions, counts):
    samples = measured[0, 0]
    tables = make_tables(probe.shape[-1])
    vmem = pl.BlockSpec(memory_space=pltpu.VMEM)
    smem = pl.BlockSpec(memory_space=pltpu.SMEM)
    layer_count, _, side, _ = object_field.shape
    tiles = (layer_count, 2, side, side)
    packed = (2, layer_count, 2, side // 2, side)
    pair = (layer_count, 2, 2, 2, side, side)
    f32 = [
        pltpu.VMEM(size, jnp.float32)
        for size in (
            packed,
            packed,
            tiles,
            (4,) + tiles,
            pair,
            pair,
            (2, 2) + tiles,
            (2,) + tiles,
            (layer_count, 2, 2, side, side),
            (layer_count, 2, 2, side, side),
            packed,
            packed,
            (2, layer_count, side // 2, side),
        )
    ]
    return pl.pallas_call(
        functools.partial(step_kernel, shape),
        out_shape=jax.ShapeDtypeStruct(object_field.shape, jnp.float32),
        in_specs=[vmem, vmem, vmem, smem, smem, pl.BlockSpec(memory_space=pltpu.HBM)],
        out_specs=vmem,
        scratch_shapes=[
            pltpu.VMEM(tables.shape, jnp.bfloat16),
            pltpu.VMEM((2,) + tiles, jnp.float32),
            pltpu.VMEM((2,) + samples.shape, jnp.float32),
            pltpu.SMEM((2,) + positions.shape[2:], jnp.int32),
            pltpu.SMEM((2,) + counts.shape, jnp.int32),
        ]
        + f32
        + [
            pltpu.SemaphoreType.DMA((COPIES,)),
            pltpu.SemaphoreType.DMA((COPIES,)),
            pltpu.SemaphoreType.DMA,
        ],
        compiler_params=pltpu.CompilerParams(collective_id=0, has_side_effects=True),
        name="steps",
    )(object_field, probe, samples, positions, counts, jnp.asarray(tables))


def solution(mesh):
    placed = (
        P(None, None, "row", "col"),
        P(),
        P("row", "col", None, None, None),
        P("row", "col", None, None),
        P("row", "col"),
    )
    return jax.shard_map(
        functools.partial(shards, dict(mesh.shape)),
        mesh=mesh,
        in_specs=placed,
        out_specs=P(None, None, "row", "col"),
        check_vma=False,
    )
```

```python
import functools

import jax
import jax.numpy as jnp
import ml_dtypes
import numpy as np
from jax import lax
from jax.experimental import pallas as pl
from jax.experimental.pallas import tpu as pltpu
from jax.sharding import PartitionSpec as P

LEARNING_RATE = 0.02
COPIES = 192


def halves_of(matrix):
    block = np.block([[matrix.real, matrix.imag], [-matrix.imag, matrix.real]])
    block = block.astype(np.float32)
    lead = block.astype(ml_dtypes.bfloat16)
    trail = (block - lead.astype(np.float32)).astype(ml_dtypes.bfloat16)
    return np.stack([lead, trail])


def make_tables(side):
    ordinal = np.arange(side)
    fourier = np.exp(-2j * np.pi / side * (np.outer(ordinal, ordinal) % side)) / np.sqrt(side)
    frequency = (ordinal + side // 2) % side - side // 2
    phase = np.exp(-0.25j * np.pi / side * frequency * frequency)
    spread = (fourier.conj() * phase[None, :]) @ fourier
    forms = [fourier, fourier.conj(), spread, spread.conj()]
    return np.stack([halves_of(form) for form in forms])


def split(values):
    lead = values.astype(jnp.bfloat16)
    return lead, (values - lead.astype(jnp.float32)).astype(jnp.bfloat16)


def dot(left, right):
    return jnp.dot(left, right, preferred_element_type=jnp.float32)


def both_sides(waves, table, form):
    side = waves[0][0].shape[0]
    stacked = jnp.concatenate([jnp.concatenate(pair, axis=1) for pair in waves], axis=0)
    lead, trail = split(stacked)
    right = (table[form, 0], table[form, 1])
    out = dot(lead, right[0]) + dot(trail, right[0]) + dot(lead, right[1])
    count = len(waves)
    turned = jnp.concatenate(
        [
            jnp.concatenate(
                [out[w * side : (w + 1) * side, part * side : (part + 1) * side] for w in range(count)],
                axis=1,
            )
            for part in range(2)
        ],
        axis=0,
    )
    lead, trail = split(turned)
    left = (table[form ^ 1, 0], table[form ^ 1, 1])
    out = dot(left[0], lead) + dot(left[0], trail) + dot(left[1], lead)
    return [
        tuple(
            out[part * side : (part + 1) * side, w * side : (w + 1) * side] for part in range(2)
        )
        for w in range(count)
    ]


def times(a, b):
    return (a[0] * b[0] - a[1] * b[1], a[0] * b[1] + a[1] * b[0])


def conj_times(a, b):
    return (a[0] * b[0] + a[1] * b[1], a[0] * b[1] - a[1] * b[0])


def pack(tile):
    half = tile.shape[0] // 2
    lane = lax.broadcasted_iota(jnp.int32, (half, tile.shape[1]), 1)
    low, high = tile[:half], tile[half:]
    left = jnp.where(lane < half, low, pltpu.roll(high, half, 1))
    right = jnp.where(lane < half, pltpu.roll(low, half, 1), high)
    return left, right


def unpack(left, right):
    half = left.shape[0]
    lane = lax.broadcasted_iota(jnp.int32, left.shape, 1)
    low = jnp.where(lane < half, left, pltpu.roll(right, half, 1))
    high = jnp.where(lane < half, pltpu.roll(left, half, 1), right)
    return jnp.concatenate([low, high], axis=0)


def step_kernel(
    shape, field_far, probe_far, samples_far, corners, count, table_far, out,
    field, probe, samples, table, near, near_samples, near_corners, near_count, far_out, far_in, wide, tall,
    grads, grads_in, later, kept, grad_rows, grad_in, grad_cols, fold_in, relay,
    send_sem, recv_sem, load_sem,
):
    layer_count = field.shape[0]
    side = field.shape[-1]
    slots = samples.shape[0]
    half = side // 2
    slices = range(layer_count)
    row, col = lax.axis_index("row"), lax.axis_index("col")
    rows_all, cols_all = shape["row"], shape["col"]
    has_row = (row > 0, row < rows_all - 1)
    has_col = (col > 0, col < cols_all - 1)
    loads = [
        pltpu.make_async_copy(src, dst, load_sem.at[i])
        for i, (src, dst) in enumerate(
            ((field_far, field), (probe_far, probe), (table_far, table), (samples_far, samples))
        )
    ]
    for load in loads:
        load.start()
    has_far = (col > 1, col < cols_all - 2)
    parts = (pl.ds(0, half), pl.ds(half, half))
    detour = cols_all == 4
    started = []
    numbers = {}

    def both(a, b):
        return jnp.logical_and(a, b)

    def passed_on(d):
        return (col == 2 - d) if detour else None

    def outer(d):
        return col == (3 if d else 0)

    def here(there, d):
        return both(there, jnp.logical_not(passed_on(d))) if detour else there

    def copy(key, src, dst, axis="col", step=0, passes=False):
        number = numbers.setdefault(key, len(numbers))
        sent = numbers.setdefault(key + ("passed",), len(numbers)) if passes else number
        return pltpu.make_async_remote_copy(
            src_ref=src,
            dst_ref=dst,
            send_sem=send_sem.at[sent],
            recv_sem=recv_sem.at[number],
            device_id={axis: (row if axis == "row" else col) + step},
            device_id_type=pl.DeviceIdType.MESH,
        )

    def start(when, moved):
        pl.when(when)(moved.start)
        started.append((when, moved))

    def arrive(when, moved):
        pl.when(when)(moved.wait_recv)

    def chunk(ref, k):
        return ref.at[0] if k == 0 else ref.at[1, parts[k - 1]]

    def near_copy(s, k, d, step=None, src=None):
        passes = src is not None
        src = src if passes else chunk(field.at[s], k)
        dst = chunk(near.at[1 - d, s], k)
        step = step if passes else 1 if d else -1
        return copy(("near", s, k, d), src, dst, "col", step, passes)

    def lend_copy(s, d):
        return copy(("lend", s), chunk(field.at[s], 2), relay.at[0, s], "col", 2 if d else -2)

    def samples_copy(d, step=None, src=None):
        passes = src is not None
        step = step if passes else 1 if d else -1
        src = src if passes else samples
        return copy(("samples", d), src, near_samples.at[1 - d], "col", step, passes)

    def place_copies(d, step=None):
        passes = step is not None
        step = step if passes else 1 if d else -1
        src = (near_corners.at[d], near_count.at[d]) if passes else (corners.at[0, 0], count)
        dst = (near_corners.at[1 - d], near_count.at[1 - d])
        return [
            copy(("place", i, d), *pair, "col", step, passes)
            for i, pair in enumerate(zip(src, dst, strict=True))
        ]

    def far_copy(s, d):
        return copy(("far", s, d), far_out.at[d, s], far_in.at[d, s], "col", 2 if d else -2)

    def tall_copy(i, s, part, d):
        ref = (field, near.at[0], near.at[1], wide)[i]
        src, dst = ref.at[s, part, parts[d]], tall.at[i, s, part, parts[d]]
        return copy(("tall", i, s, part, d), src, dst, "row", 1 if d else -1)

    def grads_copy(s, a, d):
        rows = parts[d ^ a]
        src, dst = grads.at[s, a, :, :, rows], grads_in.at[s, 1 - a, :, :, rows]
        return copy(("grads", s, a, d), src, dst, "row", 1 if d else -1)

    def fold_rows_copy(s, b, d):
        rows = parts[1 - d]
        src, dst = grad_rows.at[s, b, :, rows], grad_in.at[s, b, :, rows]
        return copy(("fold_rows", s, b, d), src, dst, "row", 1 if d else -1)

    def fold_cols_copy(s, part, d, leg=0):
        key = ("fold_cols", s, part, d)
        src, dst = grad_cols.at[1 - d, s, part], fold_in.at[1 - d, s, part]
        step = 1 if d else -1
        if leg == 0:
            return copy(key, src, dst, "col", step)
        held = relay.at[1, s]
        if leg == 1:
            return copy(("lend_cols", s), src, held, "col", 2 * step)
        return copy(key, held, dst, "col", -step)

    barrier = pltpu.get_barrier_semaphore()
    meets = [("row", 1 if d else -1, has_row[d]) for d in range(2)]
    meets += [("col", 1 if d else -1, here(has_col[d], d)) for d in range(2)]
    meets += [("col", 2 if d else -2, has_far[d]) for d in range(2)]
    for axis, step, there in meets:

        @pl.when(there)
        def greet():
            pl.semaphore_signal(
                barrier,
                inc=1,
                device_id={axis: (row if axis == "row" else col) + step},
                device_id_type=pl.DeviceIdType.MESH,
            )

    def ship_near(s):
        for k in range(3):
            for d in range(2):
                start(here(has_col[d], d), near_copy(s, k, d))

    def ship_far(s):
        for d in range(2):
            start(has_far[d], far_copy(s, d))
            if detour:
                start(passed_on(d), lend_copy(s, d))

    def hand_lent(s):
        if detour:
            for d in range(2):
                away = outer(d)
                arrive(away, lend_copy(s, d))
                start(away, near_copy(s, 2, d, -1 if d else 1, relay.at[0, s]))

    def relayed_to(d):
        return (col == 1 + d) if detour else None

    def ship_tall(when, i, s, part, d):
        start(both(when, has_row[d]), tall_copy(i, s, part, d))

    def ship_piece(when, i, s, k):
        if k == 0:
            for d in range(2):
                ship_tall(when, i, s, 0, d)
        else:
            ship_tall(when, i, s, 1, k - 1)

    def take_direct(s):
        for k in range(3):
            for d in range(2):
                mine = has_col[1 - d]
                if detour:
                    mine = both(mine, jnp.logical_not(relayed_to(d)))
                arrive(mine, near_copy(s, k, d))
                if detour and k < 2:
                    src = chunk(near.at[1 - d, s], k)
                    start(outer(d), near_copy(s, k, 1 - d, -2 if d else 2, src))
                ship_piece(mine, 2 - d, s, k)

    def take_relayed(s):
        if detour:
            for k in range(3):
                for d in range(2):
                    mine = relayed_to(d)
                    arrive(mine, near_copy(s, k, d))
                    ship_piece(mine, 2 - d, s, k)

    def take_far(s):
        for d in range(2):
            arrive(has_far[1 - d], far_copy(s, d))
        for part in range(2):
            wide[s, part] = unpack(far_in[0, s, part], far_in[1, s, part])
        for part in range(2):
            for d in range(2):
                ship_tall(has_row[d], 3, s, part, d)

    def take_places():
        for d in range(2):
            for moved in place_copies(d):
                mine = has_col[1 - d]
                arrive(both(mine, jnp.logical_not(relayed_to(d))) if detour else mine, moved)
        if detour:
            for d in range(2):
                for moved in place_copies(1 - d, -2 if d else 2):
                    start(outer(d), moved)
            for d in range(2):
                for moved in place_copies(d):
                    arrive(relayed_to(d), moved)

    def hand_samples():
        if detour:
            for d in range(2):
                away = outer(1 - d)
                arrive(away, samples_copy(1 - d))
                start(away, samples_copy(d, 2 if d else -2, near_samples.at[d]))

    def ship_samples(mine):
        for d in range(2):
            when = here(has_col[d], d)
            start(when if mine is None else both(when, mine), samples_copy(d))

    def clear(when, *refs):
        @pl.when(jnp.logical_not(when))
        def fill():
            for ref in refs:
                ref[...] = jnp.zeros(ref.shape, ref.dtype)

    for d in range(2):
        clear(has_col[d], near.at[d], near_samples.at[d], tall.at[1 + d], fold_in.at[d])
        clear(has_far[1 - d], far_in.at[d])
        rows = parts[1 - d]
        for s in slices:
            clear(has_row[d], tall.at[0, s, :, rows], tall.at[3, s, :, rows])
            clear(has_row[d], tall.at[1, s, :, rows], tall.at[2, s, :, rows])
            clear(has_row[d], grads_in.at[s, 0, :, :, parts[d]], grads_in.at[s, 1, :, :, rows])
            clear(has_row[d], grad_in.at[s, :, :, parts[d]])

        @pl.when(jnp.logical_not(has_col[d]))
        def nobody():
            near_count[d, 0, 0] = 0
            for j in range(slots):
                for dim in range(2):
                    near_corners[d, j, dim] = 0

    lane = lax.broadcasted_iota(jnp.int32, (side, side), 1)
    first = lane < half

    class Window:
        pass

    def corner_of(k, j, dim):
        return corners[0, 0, j, dim] if k == 1 else near_corners[k // 2, j, dim]

    def window_of(k, j):
        found = Window()
        found.tile, found.slot = k, j
        masks = []
        for dim in range(2):
            place = lax.broadcasted_iota(jnp.int32, (side, side), dim)
            corner = corner_of(k, j, dim)
            masks.append((place >= corner + half) | (place < corner - half))
        found.rows, found.cols = masks
        shifts = [lax.rem(corner_of(k, j, dim) + half, side) for dim in range(2)]
        found.beam = tuple(
            pltpu.roll(pltpu.roll(probe[part], shifts[0], 0), shifts[1], 1) for part in range(2)
        )
        found.live = j < (count[0, 0] if k == 1 else near_count[k // 2, 0, 0])
        return found

    loads[0].wait()
    for s in slices:
        for part in range(2):
            for d, piece in enumerate(pack(field[s, part])):
                far_out[d, s, part] = piece
    pl.semaphore_wait(barrier, sum(there.astype(jnp.int32) for _, _, there in meets))
    for s in slices:
        if s < 2:
            ship_near(s)
        ship_far(s)
        for part in range(2):
            for d in range(2):
                ship_tall(has_row[d], 0, s, part, d)
        if s == 0:
            for d in range(2):
                for moved in place_copies(d):
                    start(here(has_col[d], d), moved)
    for load in loads[1:]:
        load.wait()
    own_windows = [window_of(1, j) for j in range(slots)]

    def land_tall(s):
        for i in range(4):
            for part in range(2):
                for d in range(2):
                    there = has_row[1 - d]
                    if i in (1, 2):
                        there = both(there, has_col[i - 1])
                    arrive(there, tall_copy(i, s, part, d))

    def spread(tiles, beyond, k):
        if k == 1:
            return jnp.where(first, tiles[2], tiles[0])
        return jnp.where(first, tiles[1], beyond) if k == 0 else jnp.where(first, beyond, tiles[1])

    def cut(w, inner, across, down, slant):
        return tuple(
            jnp.where(
                w.rows,
                jnp.where(w.cols, slant[part], down[part]),
                jnp.where(w.cols, across[part], inner[part]),
            )
            for part in range(2)
        )

    def layers_first(s, windows):
        pieces = {}
        for k in range(3):
            tiles = [[near[0, s, p], field[s, p], near[1, s, p]] for p in range(2)]
            talls = [[tall[1, s, p], tall[0, s, p], tall[2, s, p]] for p in range(2)]
            pieces[k] = (
                [tiles[p][k] for p in range(2)],
                [spread(tiles[p], wide[s, p], k) for p in range(2)],
                [talls[p][k] for p in range(2)],
                [spread(talls[p], tall[3, s, p], k) for p in range(2)],
            )
        return [cut(w, *pieces[w.tile]) for w in windows]

    def residues(far, windows):
        scaled = []
        for w, value in zip(windows, far, strict=True):
            seen = samples[w.slot] if w.tile == 1 else near_samples[w.tile // 2, w.slot]
            residue = value[0] * value[0] + value[1] * value[1] - seen
            scaled.append((residue * value[0], residue * value[1]))
        return scaled

    def gather_first(s, windows, pieces):
        keep = jnp.zeros((side, side), jnp.float32)
        for part in range(2):
            totals = [[keep, keep], [keep, keep]]
            for w, piece in zip(windows, pieces, strict=True):
                value = jnp.where(w.live, piece[part], 0.0)
                inner, outside = jnp.where(w.cols, 0.0, value), jnp.where(w.cols, value, 0.0)
                if w.tile == 0:
                    inner, outside = jnp.where(first, outside, 0.0), jnp.where(first, 0.0, inner)
                elif w.tile == 2:
                    inner, outside = jnp.where(first, 0.0, outside), jnp.where(first, inner, 0.0)
                for b, share in enumerate((inner, outside)):
                    totals[0][b] += jnp.where(w.rows, 0.0, share)
                    totals[1][b] += jnp.where(w.rows, share, 0.0)
            for a in range(2):
                for b in range(2):
                    grads[s, a, b, part] = totals[a][b]

    def send_grads(s, a):
        for d in range(2):
            start(has_row[d], grads_copy(s, a, d))

    def renew(s):
        for a in range(2):
            for d in range(2):
                arrive(has_row[1 - d], grads_copy(s, a, d))
        top = lax.broadcasted_iota(jnp.int32, (side, side), 0) < half
        in_cols = jnp.where(first, has_col[1].astype(jnp.int32), has_col[0].astype(jnp.int32)) > 0
        in_rows = jnp.where(top, has_row[1].astype(jnp.int32), has_row[0].astype(jnp.int32)) > 0
        for part in range(2):
            tiles = [near[0, s, part], field[s, part], near[1, s, part]]
            talls = [tall[1, s, part], tall[0, s, part], tall[2, s, part]]
            before = [[tiles[1], spread(tiles, None, 1)], [talls[1], spread(talls, None, 1)]]
            for a in range(2):
                for b in range(2):
                    total = grads[s, a, b, part] + grads_in[s, a, b, part]
                    value = before[a][b] - LEARNING_RATE * total
                    if b:
                        value = jnp.where(in_cols, value, 0.0)
                    if a:
                        value = jnp.where(in_rows, value, 0.0)
                    later[a, b, s, part] = value

    def layers_second(s, windows):
        pieces = [[later[a, b, s, part] for part in range(2)] for a in range(2) for b in range(2)]
        return [cut(w, *pieces) for w in windows]

    take_direct(0)
    take_far(0)
    hand_lent(0)
    for s in range(2, layer_count):
        ship_near(s)
    ends = jnp.logical_or(outer(0), outer(1))
    ship_samples(jnp.logical_not(ends) if detour else None)
    take_places()
    side_windows = [window_of(k, j) for k in (0, 2) for j in range(slots)]
    windows = own_windows + side_windows
    waves = [w.beam for w in windows]
    incident, layers = [], []
    for s in range(1, layer_count):
        if s == 1:
            take_direct(s)
        take_far(s)
        hand_lent(s)
    if detour:
        ship_samples(ends)
    take_relayed(0)
    for s in slices:
        if s + 2 < layer_count:
            take_direct(s + 2)
        if s + 1 < layer_count:
            take_relayed(s + 1)
        if s + 2 == layer_count:
            hand_samples()
        land_tall(s)
        incident.append(waves)
        layers.append(layers_first(s, windows))
        waves = [times(layer, wave) for layer, wave in zip(layers[s], waves, strict=True)]
        if s + 1 < layer_count:
            waves = both_sides(waves, table, 2)
    far = both_sides(waves, table, 0)
    for d in range(2):
        mine = has_col[1 - d]
        arrive(both(mine, jnp.logical_not(outer(d))) if detour else mine, samples_copy(d))
    back = both_sides(residues(far, windows), table, 1)
    for s in reversed(slices):
        pieces = [conj_times(a, b) for a, b in zip(incident[s], back, strict=True)]
        gather_first(s, windows, pieces)
        send_grads(s, 0)
        if s > 0:
            moved = [conj_times(a, b) for a, b in zip(layers[s], back, strict=True)]
            back = both_sides(moved, table, 3)
    for s in slices:
        send_grads(s, 1)

    windows = own_windows
    waves = [w.beam for w in windows]
    incident, layers = [], []
    for s in slices:
        renew(s)
        incident.append(waves)
        layers.append(layers_second(s, windows))
        waves = [times(layer, wave) for layer, wave in zip(layers[s], waves, strict=True)]
        if s + 1 < layer_count:
            waves = both_sides(waves, table, 2)
    far = both_sides(waves, table, 0)
    back = both_sides(residues(far, windows), table, 1)

    def gather_second(s, pieces):
        for part in range(2):
            totals = [[0.0, 0.0], [0.0, 0.0]]
            for w, piece in zip(windows, pieces, strict=True):
                value = jnp.where(w.live, piece[part], 0.0)
                by_rows = (jnp.where(w.rows, 0.0, value), jnp.where(w.rows, value, 0.0))
                for a in range(2):
                    totals[a][0] += jnp.where(w.cols, 0.0, by_rows[a])
                    totals[a][1] += jnp.where(w.cols, by_rows[a], 0.0)
            for b in range(2):
                kept[b, s, part] = totals[0][b]
                grad_rows[s, b, part] = totals[1][b]
        for d in range(2):
            start(has_row[d], fold_rows_copy(s, 1, d))

    def ship_cols(s):
        for d in range(2):
            arrive(has_row[1 - d], fold_rows_copy(s, 1, d))
        for part in range(2):
            aside = kept[1, s, part] + grad_in[s, 1, part]
            for d, piece in enumerate(pack(aside)):
                grad_cols[d, s, part] = piece
        for part in (1, 0):
            for d in range(2):
                when = here(has_col[d], d) if part else has_col[d]
                start(when, fold_cols_copy(s, part, d))
                if detour and part:
                    start(passed_on(d), fold_cols_copy(s, part, d, 1))

    def hand_cols(s):
        if detour:
            for d in range(2):
                arrive(outer(d), fold_cols_copy(s, 1, d, 1))
                start(outer(d), fold_cols_copy(s, 1, d, 2))

    def finish(s):
        for d in range(2):
            arrive(has_row[1 - d], fold_rows_copy(s, 0, d))
            for part in range(2):
                arrive(has_col[1 - d], fold_cols_copy(s, part, d))
        for part in range(2):
            inner = kept[0, s, part] + grad_in[s, 0, part]
            total = inner + unpack(fold_in[0, s, part], fold_in[1, s, part])
            out[s, part] = later[0, 0, s, part] - LEARNING_RATE * total

    for s in reversed(slices):
        gather_second(s, [conj_times(a, b) for a, b in zip(incident[s], back, strict=True)])
        if s + 1 < layer_count:
            ship_cols(s + 1)
        if s > 0:
            moved = [conj_times(a, b) for a, b in zip(layers[s], back, strict=True)]
            back = both_sides(moved, table, 3)
    for s in reversed(slices):
        for d in range(2):
            start(has_row[d], fold_rows_copy(s, 0, d))
    for s in range(layer_count - 1, 1, -1):
        hand_cols(s)
    ship_cols(0)
    for s in reversed(range(min(2, layer_count))):
        hand_cols(s)
    for s in reversed(slices):
        finish(s)
    for when, moved in started:
        pl.when(when)(moved.wait_send)
    assert len(numbers) <= COPIES


def shards(shape, object_field, probe, measured, positions, counts):
    samples = measured[0, 0]
    tables = make_tables(probe.shape[-1])
    vmem = pl.BlockSpec(memory_space=pltpu.VMEM)
    smem = pl.BlockSpec(memory_space=pltpu.SMEM)
    hbm = pl.BlockSpec(memory_space=pltpu.HBM)
    layer_count, _, side, _ = object_field.shape
    tiles = (layer_count, 2, side, side)
    packed = (2, layer_count, 2, side // 2, side)
    pair = (layer_count, 2, 2, 2, side, side)
    f32 = [
        pltpu.VMEM(size, jnp.float32)
        for size in (
            packed,
            packed,
            tiles,
            (4,) + tiles,
            pair,
            pair,
            (2, 2) + tiles,
            (2,) + tiles,
            (layer_count, 2, 2, side, side),
            (layer_count, 2, 2, side, side),
            packed,
            packed,
            (2, layer_count, side // 2, side),
        )
    ]
    return pl.pallas_call(
        functools.partial(step_kernel, shape),
        out_shape=jax.ShapeDtypeStruct(object_field.shape, jnp.float32),
        in_specs=[hbm, hbm, hbm, smem, smem, hbm],
        out_specs=vmem,
        scratch_shapes=[
            pltpu.VMEM(tiles, jnp.float32),
            pltpu.VMEM(probe.shape, jnp.float32),
            pltpu.VMEM(samples.shape, jnp.float32),
            pltpu.VMEM(tables.shape, jnp.bfloat16),
            pltpu.VMEM((2,) + tiles, jnp.float32),
            pltpu.VMEM((2,) + samples.shape, jnp.float32),
            pltpu.SMEM((2,) + positions.shape[2:], jnp.int32),
            pltpu.SMEM((2,) + counts.shape, jnp.int32),
        ]
        + f32
        + [
            pltpu.SemaphoreType.DMA((COPIES,)),
            pltpu.SemaphoreType.DMA((COPIES,)),
            pltpu.SemaphoreType.DMA((4,)),
        ],
        compiler_params=pltpu.CompilerParams(collective_id=0, has_side_effects=True),
        name="steps",
    )(object_field, probe, samples, positions, counts, jnp.asarray(tables))


def solution(mesh):
    placed = (
        P(None, None, "row", "col"),
        P(),
        P("row", "col", None, None, None),
        P("row", "col", None, None),
        P("row", "col"),
    )
    return jax.shard_map(
        functools.partial(shards, dict(mesh.shape)),
        mesh=mesh,
        in_specs=placed,
        out_specs=P(None, None, "row", "col"),
        check_vma=False,
    )
```

```python
import functools

import jax
import jax.numpy as jnp
import ml_dtypes
import numpy as np
from jax import lax
from jax.experimental import pallas as pl
from jax.experimental.pallas import tpu as pltpu
from jax.sharding import PartitionSpec as P

LEARNING_RATE = 0.02
COPIES = 192


def halves_of(matrix):
    block = np.block([[matrix.real, matrix.imag], [-matrix.imag, matrix.real]])
    block = block.astype(np.float32)
    lead = block.astype(ml_dtypes.bfloat16)
    trail = (block - lead.astype(np.float32)).astype(ml_dtypes.bfloat16)
    return np.stack([lead, trail])


def make_tables(side):
    ordinal = np.arange(side)
    fourier = np.exp(-2j * np.pi / side * (np.outer(ordinal, ordinal) % side)) / np.sqrt(side)
    frequency = (ordinal + side // 2) % side - side // 2
    phase = np.exp(-0.25j * np.pi / side * frequency * frequency)
    spread = (fourier.conj() * phase[None, :]) @ fourier
    forms = [fourier, fourier.conj(), spread, spread.conj()]
    return np.stack([halves_of(form) for form in forms])


def split(values):
    lead = values.astype(jnp.bfloat16)
    return lead, (values - lead.astype(jnp.float32)).astype(jnp.bfloat16)


def dot(left, right):
    return jnp.dot(left, right, preferred_element_type=jnp.float32)


def both_sides(waves, table, form):
    found = []
    for at in range(0, len(waves), 2):
        found += sides_of(waves[at : at + 2], table, form)
    return found


def sides_of(waves, table, form):
    side = waves[0][0].shape[0]
    stacked = jnp.concatenate([jnp.concatenate(pair, axis=1) for pair in waves], axis=0)
    lead, trail = split(stacked)
    right = (table[form, 0], table[form, 1])
    out = dot(lead, right[0]) + dot(trail, right[0]) + dot(lead, right[1])
    count = len(waves)
    turned = jnp.concatenate(
        [
            jnp.concatenate(
                [out[w * side : (w + 1) * side, part * side : (part + 1) * side] for w in range(count)],
                axis=1,
            )
            for part in range(2)
        ],
        axis=0,
    )
    lead, trail = split(turned)
    left = (table[form ^ 1, 0], table[form ^ 1, 1])
    out = dot(left[0], lead) + dot(left[0], trail) + dot(left[1], lead)
    return [
        tuple(
            out[part * side : (part + 1) * side, w * side : (w + 1) * side] for part in range(2)
        )
        for w in range(count)
    ]


def times(a, b):
    return (a[0] * b[0] - a[1] * b[1], a[0] * b[1] + a[1] * b[0])


def conj_times(a, b):
    return (a[0] * b[0] + a[1] * b[1], a[0] * b[1] - a[1] * b[0])


def pack(tile):
    half = tile.shape[0] // 2
    lane = lax.broadcasted_iota(jnp.int32, (half, tile.shape[1]), 1)
    low, high = tile[:half], tile[half:]
    left = jnp.where(lane < half, low, pltpu.roll(high, half, 1))
    right = jnp.where(lane < half, pltpu.roll(low, half, 1), high)
    return left, right


def unpack(left, right):
    half = left.shape[0]
    lane = lax.broadcasted_iota(jnp.int32, left.shape, 1)
    low = jnp.where(lane < half, left, pltpu.roll(right, half, 1))
    high = jnp.where(lane < half, pltpu.roll(left, half, 1), right)
    return jnp.concatenate([low, high], axis=0)


def step_kernel(
    shape, field_far, probe_far, samples_far, corners, count, table_far, out,
    field, probe, samples, table, near, near_samples, near_corners, near_count, far_out, far_in, wide, tall,
    grads, grads_in, later, kept, grad_rows, grad_in, grad_cols, fold_in, relay,
    send_sem, recv_sem, load_sem,
):
    layer_count = field.shape[0]
    side = field.shape[-1]
    slots = samples.shape[0]
    half = side // 2
    slices = range(layer_count)
    row, col = lax.axis_index("row"), lax.axis_index("col")
    rows_all, cols_all = shape["row"], shape["col"]
    has_row = (row > 0, row < rows_all - 1)
    has_col = (col > 0, col < cols_all - 1)
    loads = [
        pltpu.make_async_copy(src, dst, load_sem.at[i])
        for i, (src, dst) in enumerate(
            ((field_far, field), (probe_far, probe), (table_far, table), (samples_far, samples))
        )
    ]
    for load in loads:
        load.start()
    has_far = (col > 1, col < cols_all - 2)
    parts = (pl.ds(0, half), pl.ds(half, half))
    detour = cols_all == 4
    started = []
    numbers = {}

    def both(a, b):
        return jnp.logical_and(a, b)

    def passed_on(d):
        return (col == 2 - d) if detour else None

    def outer(d):
        return col == (3 if d else 0)

    def here(there, d):
        return both(there, jnp.logical_not(passed_on(d))) if detour else there

    def copy(key, src, dst, axis="col", step=0, passes=False):
        number = numbers.setdefault(key, len(numbers))
        sent = numbers.setdefault(key + ("passed",), len(numbers)) if passes else number
        return pltpu.make_async_remote_copy(
            src_ref=src,
            dst_ref=dst,
            send_sem=send_sem.at[sent],
            recv_sem=recv_sem.at[number],
            device_id={axis: (row if axis == "row" else col) + step},
            device_id_type=pl.DeviceIdType.MESH,
        )

    def start(when, moved):
        pl.when(when)(moved.start)
        started.append((when, moved))

    def arrive(when, moved):
        pl.when(when)(moved.wait_recv)

    def chunk(ref, k):
        return ref.at[0] if k == 0 else ref.at[1, parts[k - 1]]

    def near_copy(s, k, d, step=None, src=None):
        passes = src is not None
        src = src if passes else chunk(field.at[s], k)
        dst = chunk(near.at[1 - d, s], k)
        step = step if passes else 1 if d else -1
        return copy(("near", s, k, d), src, dst, "col", step, passes)

    def lend_copy(s, d):
        return copy(("lend", s), chunk(field.at[s], 2), relay.at[0, s], "col", 2 if d else -2)

    def samples_copy(d, step=None, src=None):
        passes = src is not None
        step = step if passes else 1 if d else -1
        src = src if passes else samples
        return copy(("samples", d), src, near_samples.at[1 - d], "col", step, passes)

    def place_copies(d, step=None):
        passes = step is not None
        step = step if passes else 1 if d else -1
        src = (near_corners.at[d], near_count.at[d]) if passes else (corners.at[0, 0], count)
        dst = (near_corners.at[1 - d], near_count.at[1 - d])
        return [
            copy(("place", i, d), *pair, "col", step, passes)
            for i, pair in enumerate(zip(src, dst, strict=True))
        ]

    def far_copy(s, d):
        return copy(("far", s, d), far_out.at[d, s], far_in.at[d, s], "col", 2 if d else -2)

    def tall_copy(i, s, part, d):
        ref = (field, near.at[0], near.at[1], wide)[i]
        src, dst = ref.at[s, part, parts[d]], tall.at[i, s, part, parts[d]]
        return copy(("tall", i, s, part, d), src, dst, "row", 1 if d else -1)

    def grads_copy(s, a, d):
        rows = parts[d ^ a]
        src, dst = grads.at[s, a, :, :, rows], grads_in.at[s, 1 - a, :, :, rows]
        return copy(("grads", s, a, d), src, dst, "row", 1 if d else -1)

    def fold_rows_copy(s, b, d):
        rows = parts[1 - d]
        src, dst = grad_rows.at[s, b, :, rows], grad_in.at[s, b, :, rows]
        return copy(("fold_rows", s, b, d), src, dst, "row", 1 if d else -1)

    def fold_cols_copy(s, part, d, leg=0):
        key = ("fold_cols", s, part, d)
        src, dst = grad_cols.at[1 - d, s, part], fold_in.at[1 - d, s, part]
        step = 1 if d else -1
        if leg == 0:
            return copy(key, src, dst, "col", step)
        held = relay.at[1, s]
        if leg == 1:
            return copy(("lend_cols", s), src, held, "col", 2 * step)
        return copy(key, held, dst, "col", -step)

    barrier = pltpu.get_barrier_semaphore()
    meets = [("row", 1 if d else -1, has_row[d]) for d in range(2)]
    meets += [("col", 1 if d else -1, here(has_col[d], d)) for d in range(2)]
    meets += [("col", 2 if d else -2, has_far[d]) for d in range(2)]
    for axis, step, there in meets:

        @pl.when(there)
        def greet():
            pl.semaphore_signal(
                barrier,
                inc=1,
                device_id={axis: (row if axis == "row" else col) + step},
                device_id_type=pl.DeviceIdType.MESH,
            )

    def ship_near(s):
        for k in range(3):
            for d in range(2):
                start(here(has_col[d], d), near_copy(s, k, d))

    def ship_far(s):
        for d in range(2):
            start(has_far[d], far_copy(s, d))
            if detour:
                start(passed_on(d), lend_copy(s, d))

    def hand_lent(s):
        if detour:
            for d in range(2):
                away = outer(d)
                arrive(away, lend_copy(s, d))
                start(away, near_copy(s, 2, d, -1 if d else 1, relay.at[0, s]))

    def relayed_to(d):
        return (col == 1 + d) if detour else None

    def ship_tall(when, i, s, part, d):
        start(both(when, has_row[d]), tall_copy(i, s, part, d))

    def ship_piece(when, i, s, k):
        if k == 0:
            for d in range(2):
                ship_tall(when, i, s, 0, d)
        else:
            ship_tall(when, i, s, 1, k - 1)

    def take_direct(s):
        for k in range(3):
            for d in range(2):
                mine = has_col[1 - d]
                if detour:
                    mine = both(mine, jnp.logical_not(relayed_to(d)))
                arrive(mine, near_copy(s, k, d))
                if detour and k < 2:
                    src = chunk(near.at[1 - d, s], k)
                    start(outer(d), near_copy(s, k, 1 - d, -2 if d else 2, src))
                ship_piece(mine, 2 - d, s, k)

    def take_relayed(s):
        if detour:
            for k in range(3):
                for d in range(2):
                    mine = relayed_to(d)
                    arrive(mine, near_copy(s, k, d))
                    ship_piece(mine, 2 - d, s, k)

    def take_far(s):
        for d in range(2):
            arrive(has_far[1 - d], far_copy(s, d))
        for part in range(2):
            wide[s, part] = unpack(far_in[0, s, part], far_in[1, s, part])
        for part in range(2):
            for d in range(2):
                ship_tall(has_row[d], 3, s, part, d)

    def take_places():
        for d in range(2):
            for moved in place_copies(d):
                mine = has_col[1 - d]
                arrive(both(mine, jnp.logical_not(relayed_to(d))) if detour else mine, moved)
        if detour:
            for d in range(2):
                for moved in place_copies(1 - d, -2 if d else 2):
                    start(outer(d), moved)
            for d in range(2):
                for moved in place_copies(d):
                    arrive(relayed_to(d), moved)

    def hand_samples():
        if detour:
            for d in range(2):
                away = outer(1 - d)
                arrive(away, samples_copy(1 - d))
                start(away, samples_copy(d, 2 if d else -2, near_samples.at[d]))

    def ship_samples(mine):
        for d in range(2):
            when = here(has_col[d], d)
            start(when if mine is None else both(when, mine), samples_copy(d))

    def clear(when, *refs):
        @pl.when(jnp.logical_not(when))
        def fill():
            for ref in refs:
                ref[...] = jnp.zeros(ref.shape, ref.dtype)

    for d in range(2):
        clear(has_col[d], near.at[d], near_samples.at[d], tall.at[1 + d], fold_in.at[d])
        clear(has_far[1 - d], far_in.at[d])
        rows = parts[1 - d]
        for s in slices:
            clear(has_row[d], tall.at[0, s, :, rows], tall.at[3, s, :, rows])
            clear(has_row[d], tall.at[1, s, :, rows], tall.at[2, s, :, rows])
            clear(has_row[d], grads_in.at[s, 0, :, :, parts[d]], grads_in.at[s, 1, :, :, rows])
            clear(has_row[d], grad_in.at[s, :, :, parts[d]])

        @pl.when(jnp.logical_not(has_col[d]))
        def nobody():
            near_count[d, 0, 0] = 0
            for j in range(slots):
                for dim in range(2):
                    near_corners[d, j, dim] = 0

    lane = lax.broadcasted_iota(jnp.int32, (side, side), 1)
    first = lane < half

    class Window:
        pass

    def corner_of(k, j, dim):
        return corners[0, 0, j, dim] if k == 1 else near_corners[k // 2, j, dim]

    def window_of(k, j):
        found = Window()
        found.tile, found.slot = k, j
        masks = []
        for dim in range(2):
            place = lax.broadcasted_iota(jnp.int32, (side, side), dim)
            corner = corner_of(k, j, dim)
            masks.append((place >= corner + half) | (place < corner - half))
        found.rows, found.cols = masks
        shifts = [lax.rem(corner_of(k, j, dim) + half, side) for dim in range(2)]
        found.beam = tuple(
            pltpu.roll(pltpu.roll(probe[part], shifts[0], 0), shifts[1], 1) for part in range(2)
        )
        found.live = j < (count[0, 0] if k == 1 else near_count[k // 2, 0, 0])
        return found

    loads[0].wait()
    for s in slices:
        for part in range(2):
            for d, piece in enumerate(pack(field[s, part])):
                far_out[d, s, part] = piece
    pl.semaphore_wait(barrier, sum(there.astype(jnp.int32) for _, _, there in meets))
    for s in slices:
        if s < 2:
            ship_near(s)
        ship_far(s)
        for part in range(2):
            for d in range(2):
                ship_tall(has_row[d], 0, s, part, d)
        if s == 0:
            for d in range(2):
                for moved in place_copies(d):
                    start(here(has_col[d], d), moved)
    for load in loads[1:]:
        load.wait()
    own_windows = [window_of(1, j) for j in range(slots)]

    def land_tall(s):
        for i in range(4):
            for part in range(2):
                for d in range(2):
                    there = has_row[1 - d]
                    if i in (1, 2):
                        there = both(there, has_col[i - 1])
                    arrive(there, tall_copy(i, s, part, d))

    def spread(tiles, beyond, k):
        if k == 1:
            return jnp.where(first, tiles[2], tiles[0])
        return jnp.where(first, tiles[1], beyond) if k == 0 else jnp.where(first, beyond, tiles[1])

    def cut(w, inner, across, down, slant):
        return tuple(
            jnp.where(
                w.rows,
                jnp.where(w.cols, slant[part], down[part]),
                jnp.where(w.cols, across[part], inner[part]),
            )
            for part in range(2)
        )

    def layers_first(s, windows):
        pieces = {}
        for k in range(3):
            tiles = [[near[0, s, p], field[s, p], near[1, s, p]] for p in range(2)]
            talls = [[tall[1, s, p], tall[0, s, p], tall[2, s, p]] for p in range(2)]
            pieces[k] = (
                [tiles[p][k] for p in range(2)],
                [spread(tiles[p], wide[s, p], k) for p in range(2)],
                [talls[p][k] for p in range(2)],
                [spread(talls[p], tall[3, s, p], k) for p in range(2)],
            )
        return [cut(w, *pieces[w.tile]) for w in windows]

    def residues(far, windows):
        scaled = []
        for w, value in zip(windows, far, strict=True):
            seen = samples[w.slot] if w.tile == 1 else near_samples[w.tile // 2, w.slot]
            residue = value[0] * value[0] + value[1] * value[1] - seen
            scaled.append((residue * value[0], residue * value[1]))
        return scaled

    def gather_first(s, windows, pieces):
        keep = jnp.zeros((side, side), jnp.float32)
        for part in range(2):
            totals = [[keep, keep], [keep, keep]]
            for w, piece in zip(windows, pieces, strict=True):
                value = jnp.where(w.live, piece[part], 0.0)
                inner, outside = jnp.where(w.cols, 0.0, value), jnp.where(w.cols, value, 0.0)
                if w.tile == 0:
                    inner, outside = jnp.where(first, outside, 0.0), jnp.where(first, 0.0, inner)
                elif w.tile == 2:
                    inner, outside = jnp.where(first, 0.0, outside), jnp.where(first, inner, 0.0)
                for b, share in enumerate((inner, outside)):
                    totals[0][b] += jnp.where(w.rows, 0.0, share)
                    totals[1][b] += jnp.where(w.rows, share, 0.0)
            for a in range(2):
                for b in range(2):
                    grads[s, a, b, part] = totals[a][b]

    def send_grads(s, a):
        for d in range(2):
            start(has_row[d], grads_copy(s, a, d))

    def renew(s):
        for a in range(2):
            for d in range(2):
                arrive(has_row[1 - d], grads_copy(s, a, d))
        top = lax.broadcasted_iota(jnp.int32, (side, side), 0) < half
        in_cols = jnp.where(first, has_col[1].astype(jnp.int32), has_col[0].astype(jnp.int32)) > 0
        in_rows = jnp.where(top, has_row[1].astype(jnp.int32), has_row[0].astype(jnp.int32)) > 0
        for part in range(2):
            tiles = [near[0, s, part], field[s, part], near[1, s, part]]
            talls = [tall[1, s, part], tall[0, s, part], tall[2, s, part]]
            before = [[tiles[1], spread(tiles, None, 1)], [talls[1], spread(talls, None, 1)]]
            for a in range(2):
                for b in range(2):
                    total = grads[s, a, b, part] + grads_in[s, a, b, part]
                    value = before[a][b] - LEARNING_RATE * total
                    if b:
                        value = jnp.where(in_cols, value, 0.0)
                    if a:
                        value = jnp.where(in_rows, value, 0.0)
                    later[a, b, s, part] = value

    def layers_second(s, windows):
        pieces = [[later[a, b, s, part] for part in range(2)] for a in range(2) for b in range(2)]
        return [cut(w, *pieces) for w in windows]

    take_direct(0)
    take_far(0)
    hand_lent(0)
    for s in range(2, layer_count):
        ship_near(s)
    ends = jnp.logical_or(outer(0), outer(1))
    ship_samples(jnp.logical_not(ends) if detour else None)
    take_places()
    side_windows = [window_of(k, j) for k in (0, 2) for j in range(slots)]
    windows = own_windows + side_windows
    waves = [w.beam for w in windows]
    incident, layers = [], []
    for s in range(1, layer_count):
        if s == 1:
            take_direct(s)
        take_far(s)
        hand_lent(s)
    if detour:
        ship_samples(ends)
    take_relayed(0)
    for s in slices:
        if s + 2 < layer_count:
            take_direct(s + 2)
        if s + 1 < layer_count:
            take_relayed(s + 1)
        if s + 2 == layer_count:
            hand_samples()
        land_tall(s)
        incident.append(waves)
        layers.append(layers_first(s, windows))
        waves = [times(layer, wave) for layer, wave in zip(layers[s], waves, strict=True)]
        if s + 1 < layer_count:
            waves = both_sides(waves, table, 2)
    far = both_sides(waves, table, 0)
    for d in range(2):
        mine = has_col[1 - d]
        arrive(both(mine, jnp.logical_not(outer(d))) if detour else mine, samples_copy(d))
    back = both_sides(residues(far, windows), table, 1)
    for s in reversed(slices):
        pieces = [conj_times(a, b) for a, b in zip(incident[s], back, strict=True)]
        gather_first(s, windows, pieces)
        send_grads(s, 0)
        if s > 0:
            moved = [conj_times(a, b) for a, b in zip(layers[s], back, strict=True)]
            back = both_sides(moved, table, 3)
    for s in slices:
        send_grads(s, 1)

    windows = own_windows
    waves = [w.beam for w in windows]
    incident, layers = [], []
    for s in slices:
        renew(s)
        incident.append(waves)
        layers.append(layers_second(s, windows))
        waves = [times(layer, wave) for layer, wave in zip(layers[s], waves, strict=True)]
        if s + 1 < layer_count:
            waves = both_sides(waves, table, 2)
    far = both_sides(waves, table, 0)
    back = both_sides(residues(far, windows), table, 1)

    def gather_second(s, pieces):
        for part in range(2):
            totals = [[0.0, 0.0], [0.0, 0.0]]
            for w, piece in zip(windows, pieces, strict=True):
                value = jnp.where(w.live, piece[part], 0.0)
                by_rows = (jnp.where(w.rows, 0.0, value), jnp.where(w.rows, value, 0.0))
                for a in range(2):
                    totals[a][0] += jnp.where(w.cols, 0.0, by_rows[a])
                    totals[a][1] += jnp.where(w.cols, by_rows[a], 0.0)
            for b in range(2):
                kept[b, s, part] = totals[0][b]
                grad_rows[s, b, part] = totals[1][b]
        for d in range(2):
            start(has_row[d], fold_rows_copy(s, 1, d))

    def ship_cols(s):
        for d in range(2):
            arrive(has_row[1 - d], fold_rows_copy(s, 1, d))
        for part in range(2):
            aside = kept[1, s, part] + grad_in[s, 1, part]
            for d, piece in enumerate(pack(aside)):
                grad_cols[d, s, part] = piece
        for part in (1, 0):
            for d in range(2):
                when = here(has_col[d], d) if part else has_col[d]
                start(when, fold_cols_copy(s, part, d))
                if detour and part:
                    start(passed_on(d), fold_cols_copy(s, part, d, 1))

    def hand_cols(s):
        if detour:
            for d in range(2):
                arrive(outer(d), fold_cols_copy(s, 1, d, 1))
                start(outer(d), fold_cols_copy(s, 1, d, 2))

    def finish(s):
        for d in range(2):
            arrive(has_row[1 - d], fold_rows_copy(s, 0, d))
            for part in range(2):
                arrive(has_col[1 - d], fold_cols_copy(s, part, d))
        for part in range(2):
            inner = kept[0, s, part] + grad_in[s, 0, part]
            total = inner + unpack(fold_in[0, s, part], fold_in[1, s, part])
            out[s, part] = later[0, 0, s, part] - LEARNING_RATE * total

    for s in reversed(slices):
        gather_second(s, [conj_times(a, b) for a, b in zip(incident[s], back, strict=True)])
        if s + 1 < layer_count:
            ship_cols(s + 1)
        if s > 0:
            moved = [conj_times(a, b) for a, b in zip(layers[s], back, strict=True)]
            back = both_sides(moved, table, 3)
    for s in reversed(slices):
        for d in range(2):
            start(has_row[d], fold_rows_copy(s, 0, d))
    for s in range(layer_count - 1, 1, -1):
        hand_cols(s)
    ship_cols(0)
    for s in reversed(range(min(2, layer_count))):
        hand_cols(s)
    for s in reversed(slices):
        finish(s)
    for when, moved in started:
        pl.when(when)(moved.wait_send)
    assert len(numbers) <= COPIES


def shards(shape, object_field, probe, measured, positions, counts):
    samples = measured[0, 0]
    tables = make_tables(probe.shape[-1])
    vmem = pl.BlockSpec(memory_space=pltpu.VMEM)
    smem = pl.BlockSpec(memory_space=pltpu.SMEM)
    hbm = pl.BlockSpec(memory_space=pltpu.HBM)
    layer_count, _, side, _ = object_field.shape
    tiles = (layer_count, 2, side, side)
    packed = (2, layer_count, 2, side // 2, side)
    pair = (layer_count, 2, 2, 2, side, side)
    f32 = [
        pltpu.VMEM(size, jnp.float32)
        for size in (
            packed,
            packed,
            tiles,
            (4,) + tiles,
            pair,
            pair,
            (2, 2) + tiles,
            (2,) + tiles,
            (layer_count, 2, 2, side, side),
            (layer_count, 2, 2, side, side),
            packed,
            packed,
            (2, layer_count, side // 2, side),
        )
    ]
    return pl.pallas_call(
        functools.partial(step_kernel, shape),
        out_shape=pltpu.VMEM(object_field.shape, jnp.float32),
        in_specs=[hbm, hbm, hbm, smem, smem, hbm],
        out_specs=vmem,
        scratch_shapes=[
            pltpu.VMEM(tiles, jnp.float32),
            pltpu.VMEM(probe.shape, jnp.float32),
            pltpu.VMEM(samples.shape, jnp.float32),
            pltpu.VMEM(tables.shape, jnp.bfloat16),
            pltpu.VMEM((2,) + tiles, jnp.float32),
            pltpu.VMEM((2,) + samples.shape, jnp.float32),
            pltpu.SMEM((2,) + positions.shape[2:], jnp.int32),
            pltpu.SMEM((2,) + counts.shape, jnp.int32),
        ]
        + f32
        + [
            pltpu.SemaphoreType.DMA((COPIES,)),
            pltpu.SemaphoreType.DMA((COPIES,)),
            pltpu.SemaphoreType.DMA((4,)),
        ],
        compiler_params=pltpu.CompilerParams(collective_id=0, has_side_effects=True),
        name="steps",
    )(object_field, probe, samples, positions, counts, jnp.asarray(tables))


def solution(mesh):
    placed = (
        P(None, None, "row", "col"),
        P(),
        P("row", "col", None, None, None),
        P("row", "col", None, None),
        P("row", "col"),
    )
    return jax.shard_map(
        functools.partial(shards, dict(mesh.shape)),
        mesh=mesh,
        in_specs=placed,
        out_specs=P(None, None, "row", "col"),
        check_vma=False,
    )
```

```python
import functools

import jax
import jax.numpy as jnp
import ml_dtypes
import numpy as np
from jax import lax
from jax.experimental import pallas as pl
from jax.experimental.pallas import tpu as pltpu
from jax.sharding import PartitionSpec as P

LEARNING_RATE = 0.02
COPIES = 192


def halves_of(matrix):
    block = np.block([[matrix.real, matrix.imag], [-matrix.imag, matrix.real]])
    block = block.astype(np.float32)
    lead = block.astype(ml_dtypes.bfloat16)
    trail = (block - lead.astype(np.float32)).astype(ml_dtypes.bfloat16)
    return np.stack([lead, trail])


def make_tables(side):
    ordinal = np.arange(side)
    fourier = np.exp(-2j * np.pi / side * (np.outer(ordinal, ordinal) % side)) / np.sqrt(side)
    frequency = (ordinal + side // 2) % side - side // 2
    phase = np.exp(-0.25j * np.pi / side * frequency * frequency)
    spread = (fourier.conj() * phase[None, :]) @ fourier
    forms = [fourier, fourier.conj(), spread, spread.conj()]
    return np.stack([halves_of(form) for form in forms])


def split(values):
    lead = values.astype(jnp.bfloat16)
    return lead, (values - lead.astype(jnp.float32)).astype(jnp.bfloat16)


def dot(left, right):
    return jnp.dot(left, right, preferred_element_type=jnp.float32)


def both_sides(waves, table, form):
    found = []
    for at in range(0, len(waves), 2):
        found += sides_of(waves[at : at + 2], table, form)
    return found


def sides_of(waves, table, form):
    side = waves[0][0].shape[0]
    stacked = jnp.concatenate([jnp.concatenate(pair, axis=1) for pair in waves], axis=0)
    lead, trail = split(stacked)
    right = (table[form, 0], table[form, 1])
    out = dot(lead, right[0]) + dot(trail, right[0]) + dot(lead, right[1])
    count = len(waves)
    turned = jnp.concatenate(
        [
            jnp.concatenate(
                [out[w * side : (w + 1) * side, part * side : (part + 1) * side] for w in range(count)],
                axis=1,
            )
            for part in range(2)
        ],
        axis=0,
    )
    lead, trail = split(turned)
    left = (table[form ^ 1, 0], table[form ^ 1, 1])
    out = dot(left[0], lead) + dot(left[0], trail) + dot(left[1], lead)
    return [
        tuple(
            out[part * side : (part + 1) * side, w * side : (w + 1) * side] for part in range(2)
        )
        for w in range(count)
    ]


def times(a, b):
    return (a[0] * b[0] - a[1] * b[1], a[0] * b[1] + a[1] * b[0])


def conj_times(a, b):
    return (a[0] * b[0] + a[1] * b[1], a[0] * b[1] - a[1] * b[0])


def pack(tile):
    half = tile.shape[0] // 2
    lane = lax.broadcasted_iota(jnp.int32, (half, tile.shape[1]), 1)
    low, high = tile[:half], tile[half:]
    left = jnp.where(lane < half, low, pltpu.roll(high, half, 1))
    right = jnp.where(lane < half, pltpu.roll(low, half, 1), high)
    return left, right


def unpack(left, right):
    half = left.shape[0]
    lane = lax.broadcasted_iota(jnp.int32, left.shape, 1)
    low = jnp.where(lane < half, left, pltpu.roll(right, half, 1))
    high = jnp.where(lane < half, pltpu.roll(left, half, 1), right)
    return jnp.concatenate([low, high], axis=0)


def step_kernel(
    shape, field_far, probe_far, samples_far, corners, count, table_far, out,
    field, probe, samples, table, near, near_samples, near_corners, near_count, far_out, far_in, wide, tall,
    grads, grads_in, later, kept, grad_rows, grad_in, grad_cols, fold_in, cross_out, cross_in, summed, relay,
    send_sem, recv_sem, load_sem,
):
    layer_count = field.shape[0]
    side = field.shape[-1]
    slots = samples.shape[0]
    half = side // 2
    slices = range(layer_count)
    row, col = lax.axis_index("row"), lax.axis_index("col")
    rows_all, cols_all = shape["row"], shape["col"]
    has_row = (row > 0, row < rows_all - 1)
    has_col = (col > 0, col < cols_all - 1)
    loads = [
        pltpu.make_async_copy(src, dst, load_sem.at[i])
        for i, (src, dst) in enumerate(
            ((field_far, field), (probe_far, probe), (table_far, table), (samples_far, samples))
        )
    ]
    for load in loads:
        load.start()
    has_far = (col > 1, col < cols_all - 2)
    parts = (pl.ds(0, half), pl.ds(half, half))
    detour = cols_all == 4
    started = []
    numbers = {}

    def both(a, b):
        return jnp.logical_and(a, b)

    def passed_on(d):
        return (col == 2 - d) if detour else None

    def outer(d):
        return col == (3 if d else 0)

    def here(there, d):
        return both(there, jnp.logical_not(passed_on(d))) if detour else there

    def copy(key, src, dst, axis="col", step=0, passes=False):
        number = numbers.setdefault(key, len(numbers))
        sent = numbers.setdefault(key + ("passed",), len(numbers)) if passes else number
        return pltpu.make_async_remote_copy(
            src_ref=src,
            dst_ref=dst,
            send_sem=send_sem.at[sent],
            recv_sem=recv_sem.at[number],
            device_id={axis: (row if axis == "row" else col) + step},
            device_id_type=pl.DeviceIdType.MESH,
        )

    def start(when, *moves):
        started.append((when, moves))

        @pl.when(when)
        def go():
            for moved in moves:
                moved.start()

    def arrive(when, *moves):
        @pl.when(when)
        def stay():
            for moved in moves:
                moved.wait_recv()

    def leave(count):
        for when, moves in started[:count]:

            @pl.when(when)
            def gone():
                for moved in moves:
                    moved.wait_send()

        del started[:count]

    def chunk(ref, k):
        return ref.at[0] if k == 0 else ref.at[1, parts[k - 1]]

    def near_copy(s, k, d, step=None, src=None):
        passes = src is not None
        src = src if passes else chunk(field.at[s], k)
        dst = chunk(near.at[1 - d, s], k)
        step = step if passes else 1 if d else -1
        return copy(("near", s, k, d), src, dst, "col", step, passes)

    def lend_copy(s, d):
        return copy(("lend", s), chunk(field.at[s], 2), relay.at[0, s], "col", 2 if d else -2)

    def samples_copy(d, step=None, src=None):
        passes = src is not None
        step = step if passes else 1 if d else -1
        src = src if passes else samples
        return copy(("samples", d), src, near_samples.at[1 - d], "col", step, passes)

    def place_copies(d, step=None):
        passes = step is not None
        step = step if passes else 1 if d else -1
        src = (near_corners.at[d], near_count.at[d]) if passes else (corners.at[0, 0], count)
        dst = (near_corners.at[1 - d], near_count.at[1 - d])
        return [
            copy(("place", i, d), *pair, "col", step, passes)
            for i, pair in enumerate(zip(src, dst, strict=True))
        ]

    def far_copy(s, d):
        return copy(("far", s, d), far_out.at[d, s], far_in.at[d, s], "col", 2 if d else -2)

    def tall_copy(i, s, part, d):
        ref = (field, near.at[0], near.at[1], wide)[i]
        src, dst = ref.at[s, part, parts[d]], tall.at[i, s, part, parts[d]]
        return copy(("tall", i, s, part, d), src, dst, "row", 1 if d else -1)

    def grads_copy(s, a, d):
        rows = parts[d ^ a]
        src, dst = grads.at[s, a, :, :, rows], grads_in.at[s, 1 - a, :, :, rows]
        return copy(("grads", s, a, d), src, dst, "row", 1 if d else -1)

    def fold_rows_copy(s, b, d):
        rows = parts[1 - d]
        src = grad_rows.at[s, b, :, rows]
        if s == layer_count - 1:
            src = summed.at[:, rows]
        dst = grad_in.at[s, b, :, rows]
        return copy(("fold_rows", s, b, d), src, dst, "row", 1 if d else -1)

    def fold_cols_copy(s, part, d, leg=0, cross=False):
        key = ("cross" if cross else "fold_cols", s, part, d)
        if cross:
            src, dst, held = cross_out.at[1 - d, part], cross_in.at[1 - d, part], relay.at[2, s]
        else:
            src, dst = grad_cols.at[1 - d, s, part], fold_in.at[1 - d, s, part]
            held = relay.at[1, s]
        step = 1 if d else -1
        if leg == 0:
            return copy(key, src, dst, "col", step)
        if leg == 1:
            return copy(("lend_" + key[0], s), src, held, "col", 2 * step)
        return copy(key, held, dst, "col", -step)

    barrier = pltpu.get_barrier_semaphore()
    meets = [("row", 1 if d else -1, has_row[d]) for d in range(2)]
    meets += [("col", 1 if d else -1, here(has_col[d], d)) for d in range(2)]
    meets += [("col", 2 if d else -2, has_far[d]) for d in range(2)]
    for axis, step, there in meets:

        @pl.when(there)
        def greet():
            pl.semaphore_signal(
                barrier,
                inc=1,
                device_id={axis: (row if axis == "row" else col) + step},
                device_id_type=pl.DeviceIdType.MESH,
            )

    def ship_near(s):
        for d in range(2):
            start(here(has_col[d], d), *[near_copy(s, k, d) for k in range(3)])

    def ship_far(s):
        for d in range(2):
            start(has_far[d], far_copy(s, d))
            if detour:
                start(passed_on(d), lend_copy(s, d))

    def hand_lent(s):
        if detour:
            for d in range(2):
                away = outer(d)
                arrive(away, lend_copy(s, d))
                start(away, near_copy(s, 2, d, -1 if d else 1, relay.at[0, s]))

    def relayed_to(d):
        return (col == 1 + d) if detour else None

    def piece_talls(i, s, k, d):
        if k == 0:
            return [tall_copy(i, s, 0, d)]
        return [tall_copy(i, s, 1, d)] if k - 1 == d else []

    def ship_piece(mine, i, s, k):
        for d in range(2):
            moves = piece_talls(i, s, k, d)
            if moves:
                start(both(mine, has_row[d]), *moves)

    def take_direct(s):
        for k in range(3):
            for d in range(2):
                mine = has_col[1 - d]
                if detour:
                    mine = both(mine, jnp.logical_not(relayed_to(d)))
                arrive(mine, near_copy(s, k, d))
                if detour and k < 2:
                    src = chunk(near.at[1 - d, s], k)
                    start(outer(d), near_copy(s, k, 1 - d, -2 if d else 2, src))
                ship_piece(mine, 2 - d, s, k)

    def take_relayed(s):
        if detour:
            for k in range(3):
                for d in range(2):
                    mine = relayed_to(d)
                    arrive(mine, near_copy(s, k, d))
                    ship_piece(mine, 2 - d, s, k)

    def take_far(s):
        for d in range(2):
            arrive(has_far[1 - d], far_copy(s, d))
        for part in range(2):
            wide[s, part] = unpack(far_in[0, s, part], far_in[1, s, part])
        for d in range(2):
            start(has_row[d], *[tall_copy(3, s, part, d) for part in range(2)])

    def take_places():
        for d in range(2):
            mine = has_col[1 - d]
            if detour:
                mine = both(mine, jnp.logical_not(relayed_to(d)))
            arrive(mine, *place_copies(d))
        if detour:
            for d in range(2):
                start(outer(d), *place_copies(1 - d, -2 if d else 2))
            for d in range(2):
                arrive(relayed_to(d), *place_copies(d))

    def hand_samples():
        if detour:
            for d in range(2):
                away = outer(1 - d)
                arrive(away, samples_copy(1 - d))
                start(away, samples_copy(d, 2 if d else -2, near_samples.at[d]))

    def ship_samples(mine):
        for d in range(2):
            when = here(has_col[d], d)
            start(when if mine is None else both(when, mine), samples_copy(d))

    def clear(when, *refs):
        @pl.when(jnp.logical_not(when))
        def fill():
            for ref in refs:
                ref[...] = jnp.zeros(ref.shape, ref.dtype)

    for d in range(2):
        clear(has_col[d], near.at[d], near_samples.at[d], tall.at[1 + d])
        clear(has_col[d], fold_in.at[d], cross_in.at[d])
        clear(has_far[1 - d], far_in.at[d])
        rows = parts[1 - d]
        for s in slices:
            clear(has_row[d], tall.at[0, s, :, rows], tall.at[3, s, :, rows])
            clear(has_row[d], tall.at[1, s, :, rows], tall.at[2, s, :, rows])
            clear(has_row[d], grads_in.at[s, 0, :, :, parts[d]], grads_in.at[s, 1, :, :, rows])
            clear(has_row[d], grad_in.at[s, :, :, parts[d]])

        @pl.when(jnp.logical_not(has_col[d]))
        def nobody():
            near_count[d, 0, 0] = 0
            for j in range(slots):
                for dim in range(2):
                    near_corners[d, j, dim] = 0

    lane = lax.broadcasted_iota(jnp.int32, (side, side), 1)
    first = lane < half

    class Window:
        pass

    def corner_of(k, j, dim):
        return corners[0, 0, j, dim] if k == 1 else near_corners[k // 2, j, dim]

    def window_of(k, j):
        found = Window()
        found.tile, found.slot = k, j
        masks = []
        for dim in range(2):
            place = lax.broadcasted_iota(jnp.int32, (side, side), dim)
            corner = corner_of(k, j, dim)
            masks.append((place >= corner + half) | (place < corner - half))
        found.rows, found.cols = masks
        shifts = [lax.rem(corner_of(k, j, dim) + half, side) for dim in range(2)]
        found.beam = tuple(
            pltpu.roll(pltpu.roll(probe[part], shifts[0], 0), shifts[1], 1) for part in range(2)
        )
        found.live = j < (count[0, 0] if k == 1 else near_count[k // 2, 0, 0])
        return found

    loads[0].wait()
    for s in slices:
        for part in range(2):
            for d, piece in enumerate(pack(field[s, part])):
                far_out[d, s, part] = piece
    pl.semaphore_wait(barrier, sum(there.astype(jnp.int32) for _, _, there in meets))
    for s in slices:
        if s < 2:
            ship_near(s)
        ship_far(s)
        for d in range(2):
            start(has_row[d], *[tall_copy(0, s, part, d) for part in range(2)])
        if s == 0:
            for d in range(2):
                start(here(has_col[d], d), *place_copies(d))
    for load in loads[1:]:
        load.wait()
    own_windows = [window_of(1, j) for j in range(slots)]

    def land_tall(s):
        for d in range(2):
            there = has_row[1 - d]
            arrive(there, *[tall_copy(i, s, part, d) for i in (0, 3) for part in range(2)])
            for i in (1, 2):
                there = both(has_row[1 - d], has_col[i - 1])
                arrive(there, *[tall_copy(i, s, part, d) for part in range(2)])

    def spread(tiles, beyond, k):
        if k == 1:
            return jnp.where(first, tiles[2], tiles[0])
        return jnp.where(first, tiles[1], beyond) if k == 0 else jnp.where(first, beyond, tiles[1])

    def cut(w, inner, across, down, slant):
        return tuple(
            jnp.where(
                w.rows,
                jnp.where(w.cols, slant[part], down[part]),
                jnp.where(w.cols, across[part], inner[part]),
            )
            for part in range(2)
        )

    def layers_first(s, windows):
        pieces = {}
        for k in range(3):
            tiles = [[near[0, s, p], field[s, p], near[1, s, p]] for p in range(2)]
            talls = [[tall[1, s, p], tall[0, s, p], tall[2, s, p]] for p in range(2)]
            pieces[k] = (
                [tiles[p][k] for p in range(2)],
                [spread(tiles[p], wide[s, p], k) for p in range(2)],
                [talls[p][k] for p in range(2)],
                [spread(talls[p], tall[3, s, p], k) for p in range(2)],
            )
        return [cut(w, *pieces[w.tile]) for w in windows]

    def residues(far, windows):
        scaled = []
        for w, value in zip(windows, far, strict=True):
            seen = samples[w.slot] if w.tile == 1 else near_samples[w.tile // 2, w.slot]
            residue = value[0] * value[0] + value[1] * value[1] - seen
            scaled.append((residue * value[0], residue * value[1]))
        return scaled

    def gather_first(s, windows, pieces):
        keep = jnp.zeros((side, side), jnp.float32)
        for part in range(2):
            totals = [[keep, keep], [keep, keep]]
            for w, piece in zip(windows, pieces, strict=True):
                value = jnp.where(w.live, piece[part], 0.0)
                inner, outside = jnp.where(w.cols, 0.0, value), jnp.where(w.cols, value, 0.0)
                if w.tile == 0:
                    inner, outside = jnp.where(first, outside, 0.0), jnp.where(first, 0.0, inner)
                elif w.tile == 2:
                    inner, outside = jnp.where(first, 0.0, outside), jnp.where(first, inner, 0.0)
                for b, share in enumerate((inner, outside)):
                    totals[0][b] += jnp.where(w.rows, 0.0, share)
                    totals[1][b] += jnp.where(w.rows, share, 0.0)
            for a in range(2):
                for b in range(2):
                    grads[s, a, b, part] = totals[a][b]

    def send_grads(s, a):
        for d in range(2):
            start(has_row[d], grads_copy(s, a, d))

    def renew(s):
        for d in range(2):
            arrive(has_row[1 - d], *[grads_copy(s, a, d) for a in range(2)])
        top = lax.broadcasted_iota(jnp.int32, (side, side), 0) < half
        in_cols = jnp.where(first, has_col[1].astype(jnp.int32), has_col[0].astype(jnp.int32)) > 0
        in_rows = jnp.where(top, has_row[1].astype(jnp.int32), has_row[0].astype(jnp.int32)) > 0
        for part in range(2):
            tiles = [near[0, s, part], field[s, part], near[1, s, part]]
            talls = [tall[1, s, part], tall[0, s, part], tall[2, s, part]]
            before = [[tiles[1], spread(tiles, None, 1)], [talls[1], spread(talls, None, 1)]]
            for a in range(2):
                for b in range(2):
                    total = grads[s, a, b, part] + grads_in[s, a, b, part]
                    value = before[a][b] - LEARNING_RATE * total
                    if b:
                        value = jnp.where(in_cols, value, 0.0)
                    if a:
                        value = jnp.where(in_rows, value, 0.0)
                    later[a, b, s, part] = value

    def layers_second(s, windows):
        pieces = [[later[a, b, s, part] for part in range(2)] for a in range(2) for b in range(2)]
        return [cut(w, *pieces) for w in windows]

    take_direct(0)
    take_far(0)
    hand_lent(0)
    for s in range(2, layer_count):
        ship_near(s)
    ends = jnp.logical_or(outer(0), outer(1))
    ship_samples(jnp.logical_not(ends) if detour else None)
    take_places()
    side_windows = [window_of(k, j) for k in (0, 2) for j in range(slots)]
    windows = own_windows + side_windows
    waves = [w.beam for w in windows]
    incident, layers = [], []
    for s in range(1, layer_count):
        if s == 1:
            take_direct(s)
        take_far(s)
        hand_lent(s)
    if detour:
        ship_samples(ends)
    take_relayed(0)
    for s in slices:
        if s + 2 < layer_count:
            take_direct(s + 2)
        if s + 1 < layer_count:
            take_relayed(s + 1)
        if s + 2 == layer_count:
            hand_samples()
        land_tall(s)
        incident.append(waves)
        layers.append(layers_first(s, windows))
        waves = [times(layer, wave) for layer, wave in zip(layers[s], waves, strict=True)]
        if s + 1 < layer_count:
            waves = both_sides(waves, table, 2)
    far = both_sides(waves, table, 0)
    for d in range(2):
        mine = has_col[1 - d]
        arrive(both(mine, jnp.logical_not(outer(d))) if detour else mine, samples_copy(d))
    back = both_sides(residues(far, windows), table, 1)
    early = len(started)
    for s in reversed(slices):
        pieces = [conj_times(a, b) for a, b in zip(incident[s], back, strict=True)]
        gather_first(s, windows, pieces)
        send_grads(s, 0)
        if s > 0:
            moved = [conj_times(a, b) for a, b in zip(layers[s], back, strict=True)]
            back = both_sides(moved, table, 3)
    for s in slices:
        send_grads(s, 1)
    leave(early)
    early = len(started)

    windows = own_windows
    waves = [w.beam for w in windows]
    incident, layers = [], []
    for s in slices:
        renew(s)
        incident.append(waves)
        layers.append(layers_second(s, windows))
        waves = [times(layer, wave) for layer, wave in zip(layers[s], waves, strict=True)]
        if s + 1 < layer_count:
            waves = both_sides(waves, table, 2)
    far = both_sides(waves, table, 0)
    back = both_sides(residues(far, windows), table, 1)

    def gather_second(s, pieces):
        for part in range(2):
            totals = [[0.0, 0.0], [0.0, 0.0]]
            for w, piece in zip(windows, pieces, strict=True):
                value = jnp.where(w.live, piece[part], 0.0)
                by_rows = (jnp.where(w.rows, 0.0, value), jnp.where(w.rows, value, 0.0))
                for a in range(2):
                    totals[a][0] += jnp.where(w.cols, 0.0, by_rows[a])
                    totals[a][1] += jnp.where(w.cols, by_rows[a], 0.0)
            for b in range(2):
                kept[b, s, part] = totals[0][b]
                grad_rows[s, b, part] = totals[1][b]

    def send_cols(s, cross):
        for part in (1, 0):
            for d in range(2):
                when = here(has_col[d], d) if part else has_col[d]
                start(when, fold_cols_copy(s, part, d, 0, cross))
                if detour and part:
                    start(passed_on(d), fold_cols_copy(s, part, d, 1, cross))

    def ship_cols(s, folded):
        if folded:
            for d in range(2):
                arrive(has_row[1 - d], fold_rows_copy(s, 1, d))
        for part in range(2):
            aside = kept[1, s, part] + grad_in[s, 1, part] if folded else kept[1, s, part]
            for d, piece in enumerate(pack(aside)):
                grad_cols[d, s, part] = piece
        send_cols(s, False)

    def ship_cross(s):
        for part in range(2):
            for d, piece in enumerate(pack(grad_rows[s, 1, part])):
                cross_out[d, part] = piece
        send_cols(s, True)

    def hand_cols(s, cross=False):
        if detour:
            for d in range(2):
                arrive(outer(d), fold_cols_copy(s, 1, d, 1, cross))
                start(outer(d), fold_cols_copy(s, 1, d, 2, cross))

    def send_rows(s, b):
        for d in range(2):
            start(has_row[d], fold_rows_copy(s, b, d))

    def settle(s):
        for d in range(2):
            arrive(has_col[1 - d], *[fold_cols_copy(s, part, d, 0, True) for part in range(2)])
        for part in range(2):
            summed[part] = grad_rows[s, 0, part] + unpack(cross_in[0, part], cross_in[1, part])
        send_rows(s, 0)

    def finish(s):
        for d in range(2):
            arrive(has_row[1 - d], fold_rows_copy(s, 0, d))
            arrive(has_col[1 - d], *[fold_cols_copy(s, part, d) for part in range(2)])
        for part in range(2):
            inner = kept[0, s, part] + grad_in[s, 0, part]
            total = inner + unpack(fold_in[0, s, part], fold_in[1, s, part])
            out[s, part] = later[0, 0, s, part] - LEARNING_RATE * total

    last = layer_count - 1
    for s in reversed(slices):
        gather_second(s, [conj_times(a, b) for a, b in zip(incident[s], back, strict=True)])
        if s == last:
            ship_cross(s)
            ship_cols(s, False)
        else:
            send_rows(s, 1)
        if s > 0:
            moved = [conj_times(a, b) for a, b in zip(layers[s], back, strict=True)]
            back = both_sides(moved, table, 3)
    for s in reversed(range(last)):
        send_rows(s, 0)
    hand_cols(last, True)
    hand_cols(last)
    for s in reversed(range(last)):
        ship_cols(s, True)
    leave(early)
    settle(last)
    for s in reversed(range(last)):
        hand_cols(s)
    for s in reversed(slices[:last]):
        finish(s)
    finish(last)
    leave(len(started))
    assert len(numbers) <= COPIES


def shards(shape, object_field, probe, measured, positions, counts):
    samples = measured[0, 0]
    tables = make_tables(probe.shape[-1])
    vmem = pl.BlockSpec(memory_space=pltpu.VMEM)
    smem = pl.BlockSpec(memory_space=pltpu.SMEM)
    hbm = pl.BlockSpec(memory_space=pltpu.HBM)
    layer_count, _, side, _ = object_field.shape
    tiles = (layer_count, 2, side, side)
    packed = (2, layer_count, 2, side // 2, side)
    pair = (layer_count, 2, 2, 2, side, side)
    f32 = [
        pltpu.VMEM(size, jnp.float32)
        for size in (
            packed,
            packed,
            tiles,
            (4,) + tiles,
            pair,
            pair,
            (2, 2) + tiles,
            (2,) + tiles,
            (layer_count, 2, 2, side, side),
            (layer_count, 2, 2, side, side),
            packed,
            packed,
            packed[:1] + packed[2:],
            packed[:1] + packed[2:],
            tiles[1:],
            (3, layer_count, side // 2, side),
        )
    ]
    return pl.pallas_call(
        functools.partial(step_kernel, shape),
        out_shape=pltpu.VMEM(object_field.shape, jnp.float32),
        in_specs=[hbm, hbm, hbm, smem, smem, hbm],
        out_specs=vmem,
        scratch_shapes=[
            pltpu.VMEM(tiles, jnp.float32),
            pltpu.VMEM(probe.shape, jnp.float32),
            pltpu.VMEM(samples.shape, jnp.float32),
            pltpu.VMEM(tables.shape, jnp.bfloat16),
            pltpu.VMEM((2,) + tiles, jnp.float32),
            pltpu.VMEM((2,) + samples.shape, jnp.float32),
            pltpu.SMEM((2,) + positions.shape[2:], jnp.int32),
            pltpu.SMEM((2,) + counts.shape, jnp.int32),
        ]
        + f32
        + [
            pltpu.SemaphoreType.DMA((COPIES,)),
            pltpu.SemaphoreType.DMA((COPIES,)),
            pltpu.SemaphoreType.DMA((4,)),
        ],
        compiler_params=pltpu.CompilerParams(collective_id=0, has_side_effects=True),
        name="steps",
    )(object_field, probe, samples, positions, counts, jnp.asarray(tables))


def solution(mesh):
    placed = (
        P(None, None, "row", "col"),
        P(),
        P("row", "col", None, None, None),
        P("row", "col", None, None),
        P("row", "col"),
    )
    return jax.shard_map(
        functools.partial(shards, dict(mesh.shape)),
        mesh=mesh,
        in_specs=placed,
        out_specs=P(None, None, "row", "col"),
        check_vma=False,
    )
```

```python
import functools

import jax
import jax.numpy as jnp
import ml_dtypes
import numpy as np
from jax import lax
from jax.experimental import pallas as pl
from jax.experimental.pallas import tpu as pltpu
from jax.sharding import PartitionSpec as P

LEARNING_RATE = 0.02
COPIES = 192


def halves_of(matrix):
    block = np.block([[matrix.real, matrix.imag], [-matrix.imag, matrix.real]])
    block = block.astype(np.float32)
    lead = block.astype(ml_dtypes.bfloat16)
    trail = (block - lead.astype(np.float32)).astype(ml_dtypes.bfloat16)
    return np.stack([lead, trail])


def make_tables(side):
    ordinal = np.arange(side)
    fourier = np.exp(-2j * np.pi / side * (np.outer(ordinal, ordinal) % side)) / np.sqrt(side)
    frequency = (ordinal + side // 2) % side - side // 2
    phase = np.exp(-0.25j * np.pi / side * frequency * frequency)
    spread = (fourier.conj() * phase[None, :]) @ fourier
    forms = [fourier, fourier.conj(), spread, spread.conj()]
    return np.stack([halves_of(form) for form in forms])


def split(values):
    lead = values.astype(jnp.bfloat16)
    return lead, (values - lead.astype(jnp.float32)).astype(jnp.bfloat16)


def dot(left, right):
    return jnp.dot(left, right, preferred_element_type=jnp.float32)


def both_sides(waves, table, form):
    found = []
    for at in range(0, len(waves), 2):
        found += sides_of(waves[at : at + 2], table, form)
    return found


def sides_of(waves, table, form):
    side = waves[0][0].shape[0]
    stacked = jnp.concatenate([jnp.concatenate(pair, axis=1) for pair in waves], axis=0)
    lead, trail = split(stacked)
    right = (table[form, 0], table[form, 1])
    out = dot(lead, right[0]) + dot(trail, right[0]) + dot(lead, right[1])
    count = len(waves)
    turned = jnp.concatenate(
        [
            jnp.concatenate(
                [out[w * side : (w + 1) * side, part * side : (part + 1) * side] for w in range(count)],
                axis=1,
            )
            for part in range(2)
        ],
        axis=0,
    )
    lead, trail = split(turned)
    left = (table[form ^ 1, 0], table[form ^ 1, 1])
    out = dot(left[0], lead) + dot(left[0], trail) + dot(left[1], lead)
    return [
        tuple(
            out[part * side : (part + 1) * side, w * side : (w + 1) * side] for part in range(2)
        )
        for w in range(count)
    ]


def times(a, b):
    return (a[0] * b[0] - a[1] * b[1], a[0] * b[1] + a[1] * b[0])


def conj_times(a, b):
    return (a[0] * b[0] + a[1] * b[1], a[0] * b[1] - a[1] * b[0])


def pack(tile):
    half = tile.shape[0] // 2
    lane = lax.broadcasted_iota(jnp.int32, (half, tile.shape[1]), 1)
    low, high = tile[:half], tile[half:]
    left = jnp.where(lane < half, low, pltpu.roll(high, half, 1))
    right = jnp.where(lane < half, pltpu.roll(low, half, 1), high)
    return left, right


def unpack(left, right):
    half = left.shape[0]
    lane = lax.broadcasted_iota(jnp.int32, left.shape, 1)
    low = jnp.where(lane < half, left, pltpu.roll(right, half, 1))
    high = jnp.where(lane < half, pltpu.roll(left, half, 1), right)
    return jnp.concatenate([low, high], axis=0)


def step_kernel(
    shape, field_far, probe_far, samples_far, corners, count, table_far, out,
    field, probe, samples, table, near, near_samples, near_corners, near_count, far_out, far_in, wide, tall,
    grads, grads_in, later, kept, grad_rows, grad_in, grad_cols, fold_in, cross_out, cross_in, summed, relay,
    send_sem, recv_sem, load_sem,
):
    layer_count = field.shape[0]
    side = field.shape[-1]
    slots = samples.shape[0]
    half = side // 2
    slices = range(layer_count)
    row, col = lax.axis_index("row"), lax.axis_index("col")
    rows_all, cols_all = shape["row"], shape["col"]
    has_row = (row > 0, row < rows_all - 1)
    has_col = (col > 0, col < cols_all - 1)
    loads = [
        pltpu.make_async_copy(src, dst, load_sem.at[i])
        for i, (src, dst) in enumerate(
            ((field_far, field), (probe_far, probe), (table_far, table), (samples_far, samples))
        )
    ]
    for load in loads:
        load.start()
    has_far = (col > 1, col < cols_all - 2)
    parts = (pl.ds(0, half), pl.ds(half, half))
    detour = cols_all == 4
    started = []
    numbers = {}

    def both(a, b):
        return jnp.logical_and(a, b)

    def passed_on(d):
        return (col == 2 - d) if detour else None

    def outer(d):
        return col == (3 if d else 0)

    def here(there, d):
        return both(there, jnp.logical_not(passed_on(d))) if detour else there

    def copy(key, src, dst, axis="col", step=0, passes=False):
        number = numbers.setdefault(key, len(numbers))
        sent = numbers.setdefault(key + ("passed",), len(numbers)) if passes else number
        return pltpu.make_async_remote_copy(
            src_ref=src,
            dst_ref=dst,
            send_sem=send_sem.at[sent],
            recv_sem=recv_sem.at[number],
            device_id={axis: (row if axis == "row" else col) + step},
            device_id_type=pl.DeviceIdType.MESH,
        )

    def start(when, *moves):
        started.append((when, moves))

        @pl.when(when)
        def go():
            for moved in moves:
                moved.start()

    def arrive(when, *moves):
        @pl.when(when)
        def stay():
            for moved in moves:
                moved.wait_recv()

    def leave(count):
        for when, moves in started[:count]:

            @pl.when(when)
            def gone():
                for moved in moves:
                    moved.wait_send()

        del started[:count]

    def chunk(ref, k):
        return ref.at[0] if k == 0 else ref.at[1, parts[k - 1]]

    def near_copy(s, k, d, step=None, src=None):
        passes = src is not None
        src = src if passes else chunk(field.at[s], k)
        dst = chunk(near.at[1 - d, s], k)
        step = step if passes else 1 if d else -1
        return copy(("near", s, k, d), src, dst, "col", step, passes)

    def lend_copy(s, d):
        return copy(("lend", s), chunk(field.at[s], 2), relay.at[0, s], "col", 2 if d else -2)

    def samples_copy(d, step=None, src=None):
        passes = src is not None
        step = step if passes else 1 if d else -1
        src = src if passes else samples
        return copy(("samples", d), src, near_samples.at[1 - d], "col", step, passes)

    def place_copies(d, step=None):
        passes = step is not None
        step = step if passes else 1 if d else -1
        src = (near_corners.at[d], near_count.at[d]) if passes else (corners.at[0, 0], count)
        dst = (near_corners.at[1 - d], near_count.at[1 - d])
        return [
            copy(("place", i, d), *pair, "col", step, passes)
            for i, pair in enumerate(zip(src, dst, strict=True))
        ]

    def far_copy(s, d):
        return copy(("far", s, d), far_out.at[d, s], far_in.at[d, s], "col", 2 if d else -2)

    def tall_copy(i, s, part, d):
        ref = (field, near.at[0], near.at[1], wide)[i]
        src, dst = ref.at[s, part, parts[d]], tall.at[i, s, part, parts[d]]
        return copy(("tall", i, s, part, d), src, dst, "row", 1 if d else -1)

    def grads_copy(s, a, d):
        rows = parts[d ^ a]
        src, dst = grads.at[s, a, :, :, rows], grads_in.at[s, 1 - a, :, :, rows]
        return copy(("grads", s, a, d), src, dst, "row", 1 if d else -1)

    def fold_rows_copy(s, b, d):
        rows = parts[1 - d]
        src = grad_rows.at[s, b, :, rows]
        if s == layer_count - 1:
            src = summed.at[:, rows]
        dst = grad_in.at[s, b, :, rows]
        return copy(("fold_rows", s, b, d), src, dst, "row", 1 if d else -1)

    def fold_cols_copy(s, part, d, leg=0, cross=False):
        key = ("cross" if cross else "fold_cols", s, part, d)
        if cross:
            src, dst, held = cross_out.at[1 - d, part], cross_in.at[1 - d, part], relay.at[2, s]
        else:
            src, dst = grad_cols.at[1 - d, s, part], fold_in.at[1 - d, s, part]
            held = relay.at[1, s]
        step = 1 if d else -1
        if leg == 0:
            return copy(key, src, dst, "col", step)
        if leg == 1:
            return copy(("lend_" + key[0], s), src, held, "col", 2 * step)
        return copy(key, held, dst, "col", -step)

    barrier = pltpu.get_barrier_semaphore()
    meets = [("row", 1 if d else -1, has_row[d]) for d in range(2)]
    meets += [("col", 1 if d else -1, here(has_col[d], d)) for d in range(2)]
    meets += [("col", 2 if d else -2, has_far[d]) for d in range(2)]
    for axis, step, there in meets:

        @pl.when(there)
        def greet():
            pl.semaphore_signal(
                barrier,
                inc=1,
                device_id={axis: (row if axis == "row" else col) + step},
                device_id_type=pl.DeviceIdType.MESH,
            )

    def ship_near(s):
        for d in range(2):
            start(here(has_col[d], d), *[near_copy(s, k, d) for k in range(3)])

    def ship_far(s):
        for d in range(2):
            start(has_far[d], far_copy(s, d))
            if detour:
                start(passed_on(d), lend_copy(s, d))

    def hand_lent(s):
        if detour:
            for d in range(2):
                away = outer(d)
                arrive(away, lend_copy(s, d))
                start(away, near_copy(s, 2, d, -1 if d else 1, relay.at[0, s]))

    def relayed_to(d):
        return (col == 1 + d) if detour else None

    def piece_talls(i, s, k, d):
        if k == 0:
            return [tall_copy(i, s, 0, d)]
        return [tall_copy(i, s, 1, d)] if k - 1 == d else []

    def ship_piece(mine, i, s, k):
        for d in range(2):
            moves = piece_talls(i, s, k, d)
            if moves:
                start(both(mine, has_row[d]), *moves)

    def take_direct(s):
        for k in range(3):
            for d in range(2):
                mine = has_col[1 - d]
                if detour:
                    mine = both(mine, jnp.logical_not(relayed_to(d)))
                arrive(mine, near_copy(s, k, d))
                if detour and k < 2:
                    src = chunk(near.at[1 - d, s], k)
                    start(outer(d), near_copy(s, k, 1 - d, -2 if d else 2, src))
                ship_piece(mine, 2 - d, s, k)

    def take_relayed(s):
        if detour:
            for k in range(3):
                for d in range(2):
                    mine = relayed_to(d)
                    arrive(mine, near_copy(s, k, d))
                    ship_piece(mine, 2 - d, s, k)

    def take_far(s):
        for d in range(2):
            arrive(has_far[1 - d], far_copy(s, d))
        for part in range(2):
            wide[s, part] = unpack(far_in[0, s, part], far_in[1, s, part])
        for d in range(2):
            start(has_row[d], *[tall_copy(3, s, part, d) for part in range(2)])

    def take_places():
        for d in range(2):
            mine = has_col[1 - d]
            if detour:
                mine = both(mine, jnp.logical_not(relayed_to(d)))
            arrive(mine, *place_copies(d))
        if detour:
            for d in range(2):
                start(outer(d), *place_copies(1 - d, -2 if d else 2))
            for d in range(2):
                arrive(relayed_to(d), *place_copies(d))

    def hand_samples():
        if detour:
            for d in range(2):
                away = outer(1 - d)
                arrive(away, samples_copy(1 - d))
                start(away, samples_copy(d, 2 if d else -2, near_samples.at[d]))

    def ship_samples(mine):
        for d in range(2):
            when = here(has_col[d], d)
            start(when if mine is None else both(when, mine), samples_copy(d))

    def clear(when, *refs):
        @pl.when(jnp.logical_not(when))
        def fill():
            for ref in refs:
                ref[...] = jnp.zeros(ref.shape, ref.dtype)

    for d in range(2):
        clear(has_col[d], near.at[d], near_samples.at[d], tall.at[1 + d])
        clear(has_col[d], fold_in.at[d], cross_in.at[d])
        clear(has_far[1 - d], far_in.at[d])
        rows = parts[1 - d]
        for s in slices:
            clear(has_row[d], tall.at[0, s, :, rows], tall.at[3, s, :, rows])
            clear(has_row[d], tall.at[1, s, :, rows], tall.at[2, s, :, rows])
            clear(has_row[d], grads_in.at[s, 0, :, :, parts[d]], grads_in.at[s, 1, :, :, rows])
            clear(has_row[d], grad_in.at[s, :, :, parts[d]])

        @pl.when(jnp.logical_not(has_col[d]))
        def nobody():
            near_count[d, 0, 0] = 0
            for j in range(slots):
                for dim in range(2):
                    near_corners[d, j, dim] = 0

    lane = lax.broadcasted_iota(jnp.int32, (side, side), 1)
    first = lane < half

    class Window:
        pass

    def corner_of(k, j, dim):
        return corners[0, 0, j, dim] if k == 1 else near_corners[k // 2, j, dim]

    def window_of(k, j):
        found = Window()
        found.tile, found.slot = k, j
        masks = []
        for dim in range(2):
            place = lax.broadcasted_iota(jnp.int32, (side, side), dim)
            corner = corner_of(k, j, dim)
            masks.append((place >= corner + half) | (place < corner - half))
        found.rows, found.cols = masks
        shifts = [lax.rem(corner_of(k, j, dim) + half, side) for dim in range(2)]
        found.beam = tuple(
            pltpu.roll(pltpu.roll(probe[part], shifts[0], 0), shifts[1], 1) for part in range(2)
        )
        found.live = j < (count[0, 0] if k == 1 else near_count[k // 2, 0, 0])
        return found

    loads[0].wait()
    for s in slices:
        for part in range(2):
            for d, piece in enumerate(pack(field[s, part])):
                far_out[d, s, part] = piece
    pl.semaphore_wait(barrier, sum(there.astype(jnp.int32) for _, _, there in meets))
    for s in slices:
        if s < 2:
            ship_near(s)
        ship_far(s)
        for d in range(2):
            start(has_row[d], *[tall_copy(0, s, part, d) for part in range(2)])
        if s == 0:
            for d in range(2):
                start(here(has_col[d], d), *place_copies(d))
    for load in loads[1:]:
        load.wait()
    own_windows = [window_of(1, j) for j in range(slots)]

    def land_tall(s):
        for d in range(2):
            there = has_row[1 - d]
            arrive(there, *[tall_copy(i, s, part, d) for i in (0, 3) for part in range(2)])
            for i in (1, 2):
                there = both(has_row[1 - d], has_col[i - 1])
                arrive(there, *[tall_copy(i, s, part, d) for part in range(2)])

    def spread(tiles, beyond, k):
        if k == 1:
            return jnp.where(first, tiles[2], tiles[0])
        return jnp.where(first, tiles[1], beyond) if k == 0 else jnp.where(first, beyond, tiles[1])

    def cut(w, inner, across, down, slant):
        return tuple(
            jnp.where(
                w.rows,
                jnp.where(w.cols, slant[part], down[part]),
                jnp.where(w.cols, across[part], inner[part]),
            )
            for part in range(2)
        )

    def layers_first(s, windows):
        pieces = {}
        for k in range(3):
            tiles = [[near[0, s, p], field[s, p], near[1, s, p]] for p in range(2)]
            talls = [[tall[1, s, p], tall[0, s, p], tall[2, s, p]] for p in range(2)]
            pieces[k] = (
                [tiles[p][k] for p in range(2)],
                [spread(tiles[p], wide[s, p], k) for p in range(2)],
                [talls[p][k] for p in range(2)],
                [spread(talls[p], tall[3, s, p], k) for p in range(2)],
            )
        return [cut(w, *pieces[w.tile]) for w in windows]

    def residues(far, windows):
        scaled = []
        for w, value in zip(windows, far, strict=True):
            seen = samples[w.slot] if w.tile == 1 else near_samples[w.tile // 2, w.slot]
            residue = value[0] * value[0] + value[1] * value[1] - seen
            scaled.append((residue * value[0], residue * value[1]))
        return scaled

    def gather_first(s, windows, pieces):
        keep = jnp.zeros((side, side), jnp.float32)
        for part in range(2):
            totals = [[keep, keep], [keep, keep]]
            for w, piece in zip(windows, pieces, strict=True):
                value = jnp.where(w.live, piece[part], 0.0)
                inner, outside = jnp.where(w.cols, 0.0, value), jnp.where(w.cols, value, 0.0)
                if w.tile == 0:
                    inner, outside = jnp.where(first, outside, 0.0), jnp.where(first, 0.0, inner)
                elif w.tile == 2:
                    inner, outside = jnp.where(first, 0.0, outside), jnp.where(first, inner, 0.0)
                for b, share in enumerate((inner, outside)):
                    totals[0][b] += jnp.where(w.rows, 0.0, share)
                    totals[1][b] += jnp.where(w.rows, share, 0.0)
            for a in range(2):
                for b in range(2):
                    grads[s, a, b, part] = totals[a][b]

    def send_grads(s, a):
        for d in range(2):
            start(has_row[d], grads_copy(s, a, d))

    def renew(s):
        for d in range(2):
            arrive(has_row[1 - d], *[grads_copy(s, a, d) for a in range(2)])
        top = lax.broadcasted_iota(jnp.int32, (side, side), 0) < half
        in_cols = jnp.where(first, has_col[1].astype(jnp.int32), has_col[0].astype(jnp.int32)) > 0
        in_rows = jnp.where(top, has_row[1].astype(jnp.int32), has_row[0].astype(jnp.int32)) > 0
        for part in range(2):
            tiles = [near[0, s, part], field[s, part], near[1, s, part]]
            talls = [tall[1, s, part], tall[0, s, part], tall[2, s, part]]
            before = [[tiles[1], spread(tiles, None, 1)], [talls[1], spread(talls, None, 1)]]
            for a in range(2):
                for b in range(2):
                    total = grads[s, a, b, part] + grads_in[s, a, b, part]
                    value = before[a][b] - LEARNING_RATE * total
                    if b:
                        value = jnp.where(in_cols, value, 0.0)
                    if a:
                        value = jnp.where(in_rows, value, 0.0)
                    later[a, b, s, part] = value

    def layers_second(s, windows):
        pieces = [[later[a, b, s, part] for part in range(2)] for a in range(2) for b in range(2)]
        return [cut(w, *pieces) for w in windows]

    take_direct(0)
    take_far(0)
    hand_lent(0)
    for s in range(2, layer_count):
        ship_near(s)
    ends = jnp.logical_or(outer(0), outer(1))
    ship_samples(jnp.logical_not(ends) if detour else None)
    take_places()
    side_windows = [window_of(k, j) for k in (0, 2) for j in range(slots)]
    windows = own_windows + side_windows
    waves = [w.beam for w in windows]
    incident, layers = [], []
    for s in range(1, layer_count):
        if s == 1:
            take_direct(s)
        take_far(s)
        hand_lent(s)
    if detour:
        ship_samples(ends)
    take_relayed(0)
    for s in slices:
        if s + 2 < layer_count:
            take_direct(s + 2)
        if s + 1 < layer_count:
            take_relayed(s + 1)
        if s + 2 == layer_count:
            hand_samples()
        land_tall(s)
        incident.append(waves)
        layers.append(layers_first(s, windows))
        waves = [times(layer, wave) for layer, wave in zip(layers[s], waves, strict=True)]
        if s + 1 < layer_count:
            waves = both_sides(waves, table, 2)
    far = both_sides(waves, table, 0)
    for d in range(2):
        mine = has_col[1 - d]
        arrive(both(mine, jnp.logical_not(outer(d))) if detour else mine, samples_copy(d))
    back = both_sides(residues(far, windows), table, 1)
    early = len(started)
    for s in reversed(slices):
        pieces = [conj_times(a, b) for a, b in zip(incident[s], back, strict=True)]
        gather_first(s, windows, pieces)
        send_grads(s, 0)
        if s > 0:
            moved = [conj_times(a, b) for a, b in zip(layers[s], back, strict=True)]
            back = both_sides(moved, table, 3)
    for s in slices:
        send_grads(s, 1)
    leave(early)
    early = len(started)

    windows = own_windows
    waves = [w.beam for w in windows]
    incident, layers = [], []
    for s in slices:
        renew(s)
        incident.append(waves)
        layers.append(layers_second(s, windows))
        waves = [times(layer, wave) for layer, wave in zip(layers[s], waves, strict=True)]
        if s + 1 < layer_count:
            waves = both_sides(waves, table, 2)
    far = both_sides(waves, table, 0)
    back = both_sides(residues(far, windows), table, 1)

    def gather_second(s, pieces):
        for part in range(2):
            totals = [[0.0, 0.0], [0.0, 0.0]]
            for w, piece in zip(windows, pieces, strict=True):
                value = jnp.where(w.live, piece[part], 0.0)
                by_rows = (jnp.where(w.rows, 0.0, value), jnp.where(w.rows, value, 0.0))
                for a in range(2):
                    totals[a][0] += jnp.where(w.cols, 0.0, by_rows[a])
                    totals[a][1] += jnp.where(w.cols, by_rows[a], 0.0)
            for b in range(2):
                kept[b, s, part] = totals[0][b]
                grad_rows[s, b, part] = totals[1][b]

    def send_cols(s, cross):
        if detour:
            for d in range(2):
                lent, direct = [fold_cols_copy(s, leg, d, leg, cross) for leg in (1, 0)]
                start(passed_on(d), lent, direct)
        for d in range(2):
            moves = [fold_cols_copy(s, part, d, 0, cross) for part in (1, 0)]
            start(here(has_col[d], d), *moves)

    def ship_cols(s, folded):
        if folded:
            for d in range(2):
                arrive(has_row[1 - d], fold_rows_copy(s, 1, d))
        for part in range(2):
            aside = kept[1, s, part] + grad_in[s, 1, part] if folded else kept[1, s, part]
            for d, piece in enumerate(pack(aside)):
                grad_cols[d, s, part] = piece
        send_cols(s, False)

    def ship_cross(s):
        for part in range(2):
            for d, piece in enumerate(pack(grad_rows[s, 1, part])):
                cross_out[d, part] = piece
        send_cols(s, True)

    def hand_cols(s, cross=False):
        if detour:
            for d in range(2):
                arrive(outer(d), fold_cols_copy(s, 1, d, 1, cross))
                start(outer(d), fold_cols_copy(s, 1, d, 2, cross))

    def send_rows(s, b):
        for d in range(2):
            start(has_row[d], fold_rows_copy(s, b, d))

    def settle(s):
        for d in range(2):
            arrive(has_col[1 - d], *[fold_cols_copy(s, part, d, 0, True) for part in range(2)])
        for part in range(2):
            summed[part] = grad_rows[s, 0, part] + unpack(cross_in[0, part], cross_in[1, part])
        send_rows(s, 0)

    def finish(s):
        for d in range(2):
            arrive(has_row[1 - d], fold_rows_copy(s, 0, d))
            arrive(has_col[1 - d], *[fold_cols_copy(s, part, d) for part in range(2)])
        for part in range(2):
            inner = kept[0, s, part] + grad_in[s, 0, part]
            total = inner + unpack(fold_in[0, s, part], fold_in[1, s, part])
            out[s, part] = later[0, 0, s, part] - LEARNING_RATE * total

    last = layer_count - 1
    for s in reversed(slices):
        gather_second(s, [conj_times(a, b) for a, b in zip(incident[s], back, strict=True)])
        if s == last:
            ship_cross(s)
            ship_cols(s, False)
        else:
            send_rows(s, 1)
        if s > 0:
            moved = [conj_times(a, b) for a, b in zip(layers[s], back, strict=True)]
            back = both_sides(moved, table, 3)
    for s in reversed(range(last)):
        send_rows(s, 0)
    hand_cols(last, True)
    hand_cols(last)
    for s in reversed(range(last)):
        ship_cols(s, True)
    leave(early)
    settle(last)
    for s in reversed(range(last)):
        hand_cols(s)
    for s in reversed(slices[:last]):
        finish(s)
    finish(last)
    leave(len(started))
    assert len(numbers) <= COPIES


def shards(shape, object_field, probe, measured, positions, counts):
    samples = measured[0, 0]
    tables = make_tables(probe.shape[-1])
    vmem = pl.BlockSpec(memory_space=pltpu.VMEM)
    smem = pl.BlockSpec(memory_space=pltpu.SMEM)
    hbm = pl.BlockSpec(memory_space=pltpu.HBM)
    layer_count, _, side, _ = object_field.shape
    tiles = (layer_count, 2, side, side)
    packed = (2, layer_count, 2, side // 2, side)
    pair = (layer_count, 2, 2, 2, side, side)
    f32 = [
        pltpu.VMEM(size, jnp.float32)
        for size in (
            packed,
            packed,
            tiles,
            (4,) + tiles,
            pair,
            pair,
            (2, 2) + tiles,
            (2,) + tiles,
            (layer_count, 2, 2, side, side),
            (layer_count, 2, 2, side, side),
            packed,
            packed,
            packed[:1] + packed[2:],
            packed[:1] + packed[2:],
            tiles[1:],
            (3, layer_count, side // 2, side),
        )
    ]
    return pl.pallas_call(
        functools.partial(step_kernel, shape),
        out_shape=pltpu.VMEM(object_field.shape, jnp.float32),
        in_specs=[hbm, hbm, hbm, smem, smem, hbm],
        out_specs=vmem,
        scratch_shapes=[
            pltpu.VMEM(tiles, jnp.float32),
            pltpu.VMEM(probe.shape, jnp.float32),
            pltpu.VMEM(samples.shape, jnp.float32),
            pltpu.VMEM(tables.shape, jnp.bfloat16),
            pltpu.VMEM((2,) + tiles, jnp.float32),
            pltpu.VMEM((2,) + samples.shape, jnp.float32),
            pltpu.SMEM((2,) + positions.shape[2:], jnp.int32),
            pltpu.SMEM((2,) + counts.shape, jnp.int32),
        ]
        + f32
        + [
            pltpu.SemaphoreType.DMA((COPIES,)),
            pltpu.SemaphoreType.DMA((COPIES,)),
            pltpu.SemaphoreType.DMA((4,)),
        ],
        compiler_params=pltpu.CompilerParams(collective_id=0, has_side_effects=True),
        name="steps",
    )(object_field, probe, samples, positions, counts, jnp.asarray(tables))


def solution(mesh):
    placed = (
        P(None, None, "row", "col"),
        P(),
        P("row", "col", None, None, None),
        P("row", "col", None, None),
        P("row", "col"),
    )
    return jax.shard_map(
        functools.partial(shards, dict(mesh.shape)),
        mesh=mesh,
        in_specs=placed,
        out_specs=P(None, None, "row", "col"),
        check_vma=False,
    )
```
